32 devices in a mesh: dp: 8 (over z, y), fsdp: 4 (over x, core).
Axes of the slice: x: 2, y: 2, z: 4, core: 2. Of those that a mesh axis runs over, the one named last changes fastest.
Arguments:
- tokens: bfloat16 [16384, 768], P(('dp', 'fsdp')), may hold values from -6 to 6
- valid_mask: int32 [16384], P(('dp', 'fsdp')), may hold values 0 or 1
- target: bfloat16 [16384, 768], P(('dp', 'fsdp')), may hold values from -8 to 8
- params: float32 [55552, 128], P(('dp', 'fsdp')), may hold values from -4 to 4, as said below
- first_moment: float32 [55552, 128], P(('dp', 'fsdp')), may hold values from -1 to 1, as said below
- second_moment: float32 [55552, 128], P(('dp', 'fsdp')), may hold values from 0 to 1, as said below
Outputs:
- activations: bfloat16 [16384, 768], P(('dp', 'fsdp'))
- loss: float32 [], replicated
- input_grad: float32 [16384, 768], P(('dp', 'fsdp'))
- new_params: float32 [55552, 128], P(('dp', 'fsdp'))
- new_first: float32 [55552, 128], P(('dp', 'fsdp'))
- new_second: float32 [55552, 128], P(('dp', 'fsdp'))
The draws below stay inside these ranges and needn't reach their ends.
Inputs may be any that keep to these rules, and one draw needn't show every extreme that they name: `params`: entries beyond 7087104 in row order are zero. `first_moment`: entries beyond 7087104 in row order are zero. `second_moment`: entries beyond 7087104 in row order are zero.
All inputs are finite; a program needn't handle non-finite values. No bound on the sum of `valid_mask` on one device may be relied on, other than what follows from the above.
Results may differ from the reference program's by a relative error of at most 0.012.
The reference program's roundings to bfloat16 on the way count: a program that leaves them out, or rounds other values in their place, can miss the bound.
Values may be sent and summed in bfloat16 or wider, within the bound.
A program may use at most 128 MiB of HBM per device.

```python
import math
import jax
import jax.numpy as jnp
from jax import lax

D = 768
HEADS = 12
HEAD = 64
FF = 3072
FRAMES = 16
STEP = 10
LANES = 128
TOKENS = 16384
NPARAM = 7087104
PROWS = 55552


def segment_tables():
    entries = PROWS * LANES
    index = jnp.arange(entries, dtype=jnp.int32)
    edge_one = 3 * D * D
    edge_two = edge_one + D * D
    edge_three = edge_two + D * FF
    edge_four = edge_three + D * FF
    spread = jnp.where(index < edge_one, D ** (-0.5), jnp.where(index < edge_two, (D / FRAMES) ** (-0.5), jnp.where(index < edge_three, D ** (-0.5), jnp.where(index < edge_four, FF ** (-0.5), 0.2))))
    factor = jnp.where(index < edge_one, 1.5, jnp.where(index < edge_two, 0.4, jnp.where(index < edge_three, 0.3, jnp.where(index < edge_four, 0.5, 1.0))))
    gain_flags = (index >= edge_four) & (index < edge_four + D) | (index >= edge_four + 5 * D) & (index < edge_four + 6 * D)
    used = (index < NPARAM).astype(jnp.float32)
    grad_size = factor * (4.0 / (TOKENS ** 0.5 * D))
    return (spread.astype(jnp.float32), grad_size.astype(jnp.float32), gain_flags, used)


def unit_noise(key, shape):
    return jax.random.truncated_normal(key, -4.0, 4.0, shape, jnp.float32)


def draw_target(key, part):
    row_index = jnp.arange(TOKENS, dtype=jnp.float32)[:, None]
    row_scale = 0.5 + 1.5 * row_index / TOKENS
    return (unit_noise(jax.random.fold_in(key, 11), (TOKENS, D)) * row_scale).astype(jnp.bfloat16)


def draw_params(key, part):
    spread, grad_size, gain_flags, used = segment_tables()
    entries = PROWS * LANES
    noise = unit_noise(jax.random.fold_in(key, 21), (entries,))
    gains = 1.0 + jax.random.uniform(jax.random.fold_in(key, 22), (entries,), jnp.float32, -0.4, 0.4)
    values = jnp.where(gain_flags, gains, spread * noise) * used
    return values.reshape(PROWS, LANES)


def draw_first_moment(key, part):
    spread, grad_size, gain_flags, used = segment_tables()
    entries = PROWS * LANES
    noise = unit_noise(jax.random.fold_in(key, 31), (entries,))
    return (0.11 * grad_size * noise * used).reshape(PROWS, LANES)


def draw_second_moment(key, part):
    spread, grad_size, gain_flags, used = segment_tables()
    entries = PROWS * LANES
    factor = jnp.exp(jax.random.uniform(jax.random.fold_in(key, 41), (entries,), jnp.float32, -0.6931472, 0.6931472))
    return (0.002 * grad_size * grad_size * factor * used).reshape(PROWS, LANES)


def touch_ends(result, rng, low, top_value):
    longest = result.shape.index(max(result.shape))
    spots = []
    for shift in (0, 1):
        where = [jax.random.randint(jax.random.fold_in(rng, axis), (), 0, length) for axis, length in enumerate(result.shape)]
        where[longest] = (where[longest] + shift) % result.shape[longest]
        spots.append(tuple(where))
    return result.at[spots[0]].set(low).at[spots[1]].set(top_value)


def levels(rng, shape, cuts, least, top_value):
    factor_of = 1.0
    for dim, parts in cuts:
        heights = jax.random.uniform(jax.random.fold_in(jax.random.fold_in(rng, 6), dim), (parts,), jnp.float32, least / len(cuts), top_value / len(cuts))
        factor_of = factor_of * jnp.repeat(jnp.exp(heights), shape[dim] // parts).reshape((-1,) + (1,) * (len(shape) - 1 - dim))
    return factor_of


def normal_values(stream_key, shape, scale, limit, split=(), held_as=jnp.bfloat16):
    result = scale * jax.random.normal(stream_key, shape, jnp.float32)
    if split:
        result = result * levels(stream_key, shape, split, -0.22, 0.18)
    return jnp.clip(result, -limit, limit).astype(held_as)


def setup_inputs(seed: int = 0) -> dict:
    arg_keys = jax.random.split(jax.random.key(seed), 7)
    return {
        "tokens": normal_values(arg_keys[0], (TOKENS, D), 1.0, 6.0, ((0, 32),)),
        "valid_mask": touch_ends((jax.random.randint(arg_keys[1], (TOKENS,), 0, 20) < 19).astype(jnp.int32), jax.random.fold_in(arg_keys[1], 1), 0, 1),
        "target": draw_target(jax.random.fold_in(arg_keys[6], 71), 0),
        "params": draw_params(jax.random.fold_in(arg_keys[6], 71), 0),
        "first_moment": draw_first_moment(jax.random.fold_in(arg_keys[6], 71), 0),
        "second_moment": draw_second_moment(jax.random.fold_in(arg_keys[6], 71), 0),
    }


@jax.custom_vjp
def low(v):
    return lax.optimization_barrier(v.astype(jnp.bfloat16)).astype(jnp.float32)

@jax.custom_vjp
def low_back(v):
    return v

def low_keep(v):
    return (low(v), None)

def low_pass(kept, grad):
    return (grad,)

def back_keep(v):
    return (v, None)

def back_low(kept, grad):
    return (low(grad),)
low.defvjp(low_keep, low_pass)
low_back.defvjp(back_keep, back_low)
precise = lax.Precision.HIGHEST
norm_epsilon = 1e-06
adam_epsilon = 1e-08
beta_one = 0.9
beta_two = 0.999
learn_rate = 0.1
weight_decay = 0.05

def unpack(flat):
    layout = [(D, 3 * D), (D, D), (D, FF), (D, FF)]
    pieces = []
    offset = 0
    for height, breadth in layout:
        pieces.append(flat[offset:offset + height * breadth].reshape(height, breadth))
        offset = offset + height * breadth
    for length in [D] * 8 + [FF]:
        pieces.append(flat[offset:offset + length])
        offset = offset + length
    return pieces

def layer_norm(values, gain, shift):
    center = values - lax.optimization_barrier(jnp.mean(values, -1, keepdims=True))
    spread = lax.optimization_barrier(jnp.mean(center * center, -1, keepdims=True))
    return center * lax.rsqrt(spread + norm_epsilon) * gain + shift

def forward(inputs, tiled, target_block, mask_block, denominator):
    flat = low(tiled).reshape(-1)[:NPARAM]
    w_qkv, w_proj, w_in, w_out, gain_one, shift_one, bias_query, bias_value, bias_proj, gain_two, shift_two, bias_out, bias_in = unpack(flat)
    token_rows = inputs.shape[0]
    places = token_rows // FRAMES
    normed_low = low(layer_norm(inputs, gain_one, shift_one))
    bias_all = jnp.concatenate([bias_query, jnp.zeros((D,), jnp.float32), bias_value])
    mixed = jnp.dot(normed_low, w_qkv, precision=precise) + bias_all
    mixed = low_back(low(mixed))
    heads_view = mixed.reshape(places, FRAMES, 3, HEADS, HEAD)
    queries = heads_view[:, :, 0]
    key_part = heads_view[:, :, 1]
    values = heads_view[:, :, 2]
    scores = jnp.einsum('pfhe,pghe->phfg', queries, key_part, precision=precise) * HEAD ** (-0.5)
    scores = low_back(scores)
    probs_low = low(jax.nn.softmax(scores, axis=-1))
    attended = jnp.einsum('phfg,pghe->pfhe', probs_low, values, precision=precise)
    attended = low_back(low(attended.reshape(token_rows, D)))
    branch = low_back(jnp.dot(attended, w_proj, precision=precise) + bias_proj)
    middle = inputs + branch
    normed_two_low = low(layer_norm(middle, gain_two, shift_two))
    hidden = low_back(jnp.dot(normed_two_low, w_in, precision=precise) + bias_in)
    active_low = low(jax.nn.gelu(hidden, approximate=False))
    second_branch = low_back(jnp.dot(active_low, w_out.T, precision=precise) + bias_out)
    output = middle + second_branch
    misfit = output - target_block
    squares = jnp.sum(mask_block * lax.optimization_barrier(jnp.sum(misfit * misfit, -1)))
    return (squares / denominator, output)

def reference(tokens, valid_mask, target, params, first_moment, second_moment):
    valid_total = jnp.sum(valid_mask.astype(jnp.float32))
    denominator = valid_total * D
    block_rows = math.gcd(TOKENS, 4096)
    blocks = TOKENS // block_rows
    inputs_all = tokens.astype(jnp.float32).reshape(blocks, block_rows, D)
    target_all = target.astype(jnp.float32).reshape(blocks, block_rows, D)
    mask_all = valid_mask.astype(jnp.float32).reshape(blocks, block_rows)

    def advance(running, block_piece):
        grad_sum, loss_sum = running
        inputs, target_block, mask_block = block_piece

        def local_loss(input_values, tiled):
            return forward(input_values, tiled, target_block, mask_block, denominator)
        (block_loss, output), pull = jax.vjp(local_loss, inputs, params)
        grad_inputs, grad_tiled = pull((jnp.ones((), jnp.float32), jnp.zeros_like(output)))
        return ((grad_sum + grad_tiled, loss_sum + block_loss), (output.astype(jnp.bfloat16), grad_inputs))
    start_state = (jnp.zeros_like(params), jnp.zeros((), jnp.float32))
    (gradient, loss), (outputs, grad_inputs) = lax.scan(advance, start_state, (inputs_all, target_all, mask_all))
    activations = outputs.reshape(TOKENS, D)
    input_grad = grad_inputs.reshape(TOKENS, D) * (TOKENS * D)
    new_first = beta_one * first_moment + (1.0 - beta_one) * gradient
    new_second = beta_two * second_moment + (1.0 - beta_two) * gradient * gradient
    first_hat = new_first / (1.0 - beta_one ** STEP)
    second_hat = new_second / (1.0 - beta_two ** STEP)
    new_params = params - learn_rate * (first_hat / (jnp.sqrt(second_hat) + adam_epsilon) + weight_decay * params)
    return (activations, loss, input_grad, new_params, new_first, new_second)
```

```python
import jax
import jax.numpy as jnp
from jax import lax
from jax.sharding import PartitionSpec as P

D = 768
HEADS = 12
HEAD = 64
FF = 3072
FRAMES = 16
STEP = 10


norm_epsilon = 1e-06
adam_epsilon = 1e-08
beta_one = 0.9
beta_two = 0.999
learn_rate = 0.1
weight_decay = 0.05


def unpack(tiled):
    flat = tiled.reshape(-1)
    layout = [(D, 3 * D), (D, D), (D, FF), (D, FF)]
    pieces = []
    offset = 0
    for height, breadth in layout:
        pieces.append(flat[offset : offset + height * breadth].reshape(height, breadth))
        offset = offset + height * breadth
    for length in [D] * 8 + [FF]:
        pieces.append(flat[offset : offset + length].astype(jnp.float32))
        offset = offset + length
    return pieces


def layer_norm(values, gain, shift):
    center = values - jnp.mean(values, -1, keepdims=True)
    spread = jnp.mean(center * center, -1, keepdims=True)
    return center * lax.rsqrt(spread + norm_epsilon) * gain + shift


def exact_gelu(values):
    return jax.nn.gelu(values, approximate=False)


def collect(shard):
    lowered = shard.astype(jnp.bfloat16)
    whole = lax.all_gather(lowered, ("dp", "fsdp"), axis=0, tiled=True)
    return whole


def reduce_rows(full):
    summed = lax.psum_scatter(
        full.astype(jnp.bfloat16), ("dp", "fsdp"), scatter_dimension=0, tiled=True
    )
    return summed.astype(jnp.float32)


def contract_rows(left, right):
    return lax.dot_general(
        left, right, (((0,), (0,)), ((), ())), preferred_element_type=jnp.float32
    )


def contract_cols(left, right):
    return lax.dot_general(
        left, right, (((1,), (1,)), ((), ())), preferred_element_type=jnp.float32
    )


def column_sum(values):
    return jnp.sum(values.astype(jnp.float32), 0)


def shards(tokens, valid_mask, target, params, first_moment, second_moment):
    token_rows = tokens.shape[0]
    places = token_rows // FRAMES
    devices = lax.axis_size("dp") * lax.axis_size("fsdp")
    lane_count = params.shape[1]
    total_rows = params.shape[0] * devices
    score_scale = HEAD ** (-0.5)
    mask_values = valid_mask.astype(jnp.float32)
    gathered = collect(params)
    (
        w_qkv,
        w_proj,
        w_in,
        w_out,
        gain_one,
        shift_one,
        bias_query,
        bias_value,
        bias_proj,
        gain_two,
        shift_two,
        bias_out,
        bias_in,
    ) = unpack(gathered)
    inputs = tokens.astype(jnp.float32)
    normed_low = layer_norm(inputs, gain_one, shift_one).astype(jnp.bfloat16)
    bias_all = jnp.concatenate([bias_query, jnp.zeros_like(bias_query), bias_value])
    mixed_low = (jnp.dot(normed_low, w_qkv, preferred_element_type=jnp.float32) + bias_all).astype(
        jnp.bfloat16
    )
    heads_view = mixed_low.reshape(places, FRAMES, 3, HEADS, HEAD)
    queries = heads_view[:, :, 0]
    key_part = heads_view[:, :, 1]
    values = heads_view[:, :, 2]
    scores = (
        jnp.einsum("pfhe,pghe->phfg", queries, key_part, preferred_element_type=jnp.float32)
        * score_scale
    )
    row_max = jnp.max(scores, -1, keepdims=True)
    log_total = row_max + jnp.log(jnp.sum(jnp.exp(scores - row_max), -1, keepdims=True))
    probs = jnp.exp(scores - log_total)
    probs_low = probs.astype(jnp.bfloat16)
    attended = jnp.einsum("phfg,pghe->pfhe", probs_low, values, preferred_element_type=jnp.float32)
    attended_low = attended.reshape(token_rows, D).astype(jnp.bfloat16)
    branch = jnp.dot(attended_low, w_proj, preferred_element_type=jnp.float32) + bias_proj
    middle = inputs + branch
    normed_two_low = layer_norm(middle, gain_two, shift_two).astype(jnp.bfloat16)
    hidden = jnp.dot(normed_two_low, w_in, preferred_element_type=jnp.float32) + bias_in
    active_low = exact_gelu(hidden).astype(jnp.bfloat16)
    second_branch = contract_cols(active_low, w_out) + bias_out
    output = middle + second_branch
    misfit = output - target.astype(jnp.float32)
    squares = jnp.sum(mask_values * jnp.sum(misfit * misfit, -1))
    total_error, kept_count = lax.psum((squares, jnp.sum(mask_values)), ("dp", "fsdp"))
    denominator = kept_count * D
    grad_out = 2.0 / denominator * mask_values[:, None] * misfit
    regathered = collect(params)
    w_qkv, w_proj, w_in, w_out = unpack(regathered)[:4]
    grad_out_low = grad_out.astype(jnp.bfloat16)
    grad_bias_out = column_sum(grad_out_low)
    grad_w_out = contract_rows(grad_out_low, active_low)
    grad_active = jnp.dot(grad_out_low, w_out, preferred_element_type=jnp.float32)
    gelu_value, gelu_pull = jax.vjp(exact_gelu, hidden)
    grad_hidden_low = gelu_pull(grad_active)[0].astype(jnp.bfloat16)
    grad_bias_in = column_sum(grad_hidden_low)
    grad_w_in = contract_rows(normed_two_low, grad_hidden_low)
    grad_normed_two = contract_cols(grad_hidden_low, w_in)
    norm_value, second_pull = jax.vjp(layer_norm, middle, gain_two, shift_two)
    grad_middle_norm, grad_gain_two, grad_shift_two = second_pull(grad_normed_two)
    grad_middle = grad_out + grad_middle_norm
    grad_branch_low = grad_middle.astype(jnp.bfloat16)
    grad_bias_proj = column_sum(grad_branch_low)
    grad_w_proj = contract_rows(attended_low, grad_branch_low)
    grad_attended_low = (
        contract_cols(grad_branch_low, w_proj)
        .astype(jnp.bfloat16)
        .reshape(places, FRAMES, HEADS, HEAD)
    )
    grad_values = jnp.einsum(
        "phfg,pfhe->pghe", probs_low, grad_attended_low, preferred_element_type=jnp.float32
    )
    grad_probs = jnp.einsum(
        "pfhe,pghe->phfg", grad_attended_low, values, preferred_element_type=jnp.float32
    )
    grad_scores_low = (
        probs * (grad_probs - jnp.sum(probs * grad_probs, -1, keepdims=True))
    ).astype(jnp.bfloat16)
    grad_queries = (
        jnp.einsum("phfg,pghe->pfhe", grad_scores_low, key_part, preferred_element_type=jnp.float32)
        * score_scale
    )
    grad_keys = (
        jnp.einsum("phfg,pfhe->pghe", grad_scores_low, queries, preferred_element_type=jnp.float32)
        * score_scale
    )
    grad_mixed_low = (
        jnp.stack([grad_queries, grad_keys, grad_values], 2)
        .reshape(token_rows, 3 * D)
        .astype(jnp.bfloat16)
    )
    grad_bias_query = column_sum(grad_mixed_low[:, :D])
    grad_bias_value = column_sum(grad_mixed_low[:, 2 * D :])
    grad_w_qkv = contract_rows(normed_low, grad_mixed_low)
    grad_normed_one = contract_cols(grad_mixed_low, w_qkv)
    first_value, first_pull = jax.vjp(layer_norm, inputs, gain_one, shift_one)
    grad_inputs_norm, grad_gain_one, grad_shift_one = first_pull(grad_normed_one)
    grad_inputs = grad_middle + grad_inputs_norm
    used_grad = jnp.concatenate(
        [
            grad_w_qkv.reshape(-1),
            grad_w_proj.reshape(-1),
            grad_w_in.reshape(-1),
            grad_w_out.reshape(-1),
            grad_gain_one,
            grad_shift_one,
            grad_bias_query,
            grad_bias_value,
            grad_bias_proj,
            grad_gain_two,
            grad_shift_two,
            grad_bias_out,
            grad_bias_in,
        ]
    )
    padding = jnp.zeros((total_rows * lane_count - used_grad.shape[0],), jnp.float32)
    whole_grad = jnp.concatenate([used_grad, padding]).reshape(total_rows, lane_count)
    gradient = reduce_rows(whole_grad)
    loss = total_error / denominator
    new_first = beta_one * first_moment + (1.0 - beta_one) * gradient
    new_second = beta_two * second_moment + (1.0 - beta_two) * gradient * gradient
    first_hat = new_first / (1.0 - beta_one**STEP)
    second_hat = new_second / (1.0 - beta_two**STEP)
    new_params = params - learn_rate * (
        first_hat / (jnp.sqrt(second_hat) + adam_epsilon) + weight_decay * params
    )
    input_grad = grad_inputs * float(token_rows * devices * D)
    return (output.astype(jnp.bfloat16), loss, input_grad, new_params, new_first, new_second)


def solution(mesh):
    return jax.shard_map(
        shards,
        mesh=mesh,
        in_specs=(
            P(("dp", "fsdp"), None),
            P(("dp", "fsdp")),
            P(("dp", "fsdp"), None),
            P(("dp", "fsdp"), None),
            P(("dp", "fsdp"), None),
            P(("dp", "fsdp"), None),
        ),
        out_specs=(
            P(("dp", "fsdp"), None),
            P(),
            P(("dp", "fsdp"), None),
            P(("dp", "fsdp"), None),
            P(("dp", "fsdp"), None),
            P(("dp", "fsdp"), None),
        ),
        check_vma=False,
    )
```

```python
import functools

import jax
import jax.numpy as jnp
from jax import lax
from jax.experimental import pallas as pl
from jax.experimental.pallas import tpu as pltpu
from jax.sharding import PartitionSpec as P

D = 768
HEADS = 12
HEAD = 64
FF = 3072
FRAMES = 16
STEP = 10


MESH = pl.DeviceIdType.MESH
NA, NB, NX = 4, 2, 2
ORDERS = ((0, 1, 2), (0, 2, 1), (1, 2, 0))


def coords():
    dp = lax.axis_index("dp")
    fs = lax.axis_index("fsdp")
    return (dp // NB, dp % NB, fs // 2), fs % 2


def device(pos, core):
    return (pos[0] * NB + pos[1], pos[2] * 2 + core)


def flat(pos, core):
    return ((pos[0] * NB + pos[1]) * NX + pos[2]) * 2 + core


def steps():
    out = []
    for da in range(-(NA - 1), NA):
        for db in range(2):
            for dx in range(2):
                out.append((abs(da) + db + dx, (da, db, dx)))
    out.sort(key=lambda t: t[0])
    return [r for _, r in out]


def children(rel, order, pos):
    last = -1
    for i, d in enumerate(order):
        if rel[d] != 0:
            last = i
    res = []

    def line(up):
        a = pos[0]
        if up:
            return (a + 1 < NA, (a + 1, pos[1], pos[2]), 0)
        return (a - 1 >= 0, (a - 1, pos[1], pos[2]), 1)

    def flip(d):
        p = list(pos)
        p[d] = 1 - p[d]
        return (None, tuple(p), 1 + d)

    if last >= 0 and order[last] == 0:
        res.append(line(rel[0] < 0))
    for i in range(last + 1, 3):
        d = order[i]
        if d == 0:
            res.append(line(True))
            res.append(line(False))
        else:
            res.append(flip(d))
    return res


def source_of(rel, pos):
    a = pos[0] + rel[0]
    valid = None
    if rel[0] > 0:
        valid = a < NA
    if rel[0] < 0:
        valid = a >= 0
    return valid, (a, (pos[1] + rel[1]) % 2, (pos[2] + rel[2]) % 2)


def when(cond, fn):
    if cond is None:
        fn()
    else:
        pl.when(cond)(fn)


def both(a, b):
    if a is None:
        return b
    if b is None:
        return a
    return jnp.logical_and(a, b)


def split_rows(rows, shares):
    tiles = rows // 16
    first = int(round(tiles * shares))
    return ((0, first * 16), (first * 16, first * 16), (2 * first * 16, rows - 2 * first * 16))


F32, BF16 = jnp.float32, jnp.bfloat16
SHARE = 0.389


def greet(pos, core):
    sem = pltpu.get_barrier_semaphore()
    a, b, x = pos
    fixed = [device(pos, 1 - core), device((a, 1 - b, x), core), device((a, b, 1 - x), core),
             device(((a + 2) % NA, b, x), core)]
    for d in fixed:
        pl.semaphore_signal(sem, inc=1, device_id=d, device_id_type=MESH)
    up, down = a + 1 < NA, a - 1 >= 0
    when(up, lambda: pl.semaphore_signal(sem, inc=1, device_id=device((a + 1, b, x), core), device_id_type=MESH))
    when(down, lambda: pl.semaphore_signal(sem, inc=1, device_id=device((a - 1, b, x), core), device_id_type=MESH))
    pl.semaphore_wait(sem, len(fixed) + up.astype(jnp.int32) + down.astype(jnp.int32))


class Total:
    def __init__(self, pos, core, buf, send, recv):
        a, b, x = pos
        flip = a + 1 - 2 * (a % 2)
        partners = [device(pos, 1 - core), device((a, b, 1 - x), core), device((a, 1 - b, x), core),
                    device((flip, b, x), core), device(((a + 2) % NA, b, x), core)]
        self.buf = buf
        self.copies = [pltpu.make_async_remote_copy(
            src_ref=buf.at[2 * i], dst_ref=buf.at[2 * i + 1], send_sem=send.at[i], recv_sem=recv.at[i],
            device_id=p, device_id_type=MESH) for i, p in enumerate(partners)]
        self.n = len(partners)

    def start(self, i):
        self.copies[i].start()

    def end(self, i):
        self.copies[i].wait()
        self.buf[2 * i + 2] = self.buf[2 * i] + self.buf[2 * i + 1]

    def hooks(self, first, gap):
        table = {}
        for i in range(self.n):
            table.setdefault(first + i * gap, []).append(functools.partial(self.start, i))
            table.setdefault(first + i * gap + gap - 2, []).append(functools.partial(self.end, i))
        return table


def gather_kernel(parts, rows, mats, own_ref, count_ref, *refs):
    nm = len(mats)
    outs, vec_ref, total_ref = refs[:nm], refs[nm], refs[nm + 1]
    slots, flat_ref, send, recv, tbuf, tsend, trecv, osem = refs[nm + 2:nm + 10]
    mat_refs = refs[nm + 10:]
    pos, core = coords()
    me = flat(pos, core)
    slots[me, 0:rows, :] = own_ref[...].astype(BF16)
    if slots.shape[1] > rows:
        slots[me, rows:, :] = jnp.zeros((slots.shape[1] - rows, 128), BF16)
    tbuf[0] = count_ref[...]
    total = Total(pos, core, tbuf, tsend, trecv)
    greet(pos, core)
    hooks = total.hooks(6, 14)
    plan = steps()
    order_k = []
    for rel in plan:
        for col in range(3):
            order_k.append((rel, col))

    def chunk(idx, col):
        lo, n = parts[col]
        return slots.at[idx, pl.ds(lo, n), :]

    def copy(idx, col, k, direction, to):
        return pltpu.make_async_remote_copy(
            src_ref=chunk(idx, col), dst_ref=chunk(idx, col),
            send_sem=send.at[k, direction], recv_sem=recv.at[idx, col],
            device_id=to, device_id_type=MESH)

    def widen(idx):
        base = pl.multiple_of(idx * rows, 8)
        def body(i, _):
            r = pl.multiple_of(i * 112, 16)
            flat_ref[pl.ds(pl.multiple_of(base + r, 8), 112), :] = slots[idx, pl.ds(r, 112), :].astype(F32)
            return 0
        lax.fori_loop(0, rows // 112, body, 0)
        rest = rows % 112
        if rest:
            r = rows // 112 * 112
            flat_ref[pl.ds(pl.multiple_of(base + r, 8), rest), :] = slots[idx, r:r + rest, :].astype(F32)

    def run(k, rel, col, valid, src):
        def inner():
            idx = flat(src, core)
            if rel != (0, 0, 0):
                copy(idx, col, k, 0, device(pos, 1 - core)).wait_recv()
            for cond, child, direction in children(rel, ORDERS[col], pos):
                when(cond, lambda child=child, direction=direction: copy(idx, col, k, direction, device(child, core)).start())
            copy(idx, col, k, 4, device(pos, 1 - core)).start()
        when(valid, inner)

    def sibling(rel, k0):
        valid, src = source_of(rel, pos)
        def inner():
            other = flat(src, 1 - core)
            for col in range(3):
                copy(other, col, k0 + col, 4, device(pos, 1 - core)).wait_recv()
            widen(flat(src, core))
            widen(other)
        when(valid, inner)

    def finish(k, rel, col, valid, src):
        def inner():
            idx = flat(src, core)
            for cond, child, direction in children(rel, ORDERS[col], pos):
                when(cond, lambda child=child, direction=direction: copy(idx, col, k, direction, device(child, core)).wait_send())
            copy(idx, col, k, 4, device(pos, 1 - core)).wait_send()
        when(valid, inner)

    LAG = 2
    for i, rel in enumerate(plan):
        valid, src = source_of(rel, pos)
        for col in range(3):
            k = 3 * i + col
            run(k, rel, col, valid, src)
            for h in hooks.get(k, ()):
                h()
        if i >= LAG:
            sibling(plan[i - LAG], 3 * (i - LAG))
    for i in range(len(plan) - LAG, len(plan)):
        sibling(plan[i], 3 * i)
    total_ref[...] = tbuf[2 * total.n]
    first = 0
    copies = []
    for (height, width), mat, out, s in zip(mats, mat_refs, outs, range(nm)):
        n = width // 128
        def body(i, _, mat=mat, n=n, first=first):
            r = pl.multiple_of(i * 16, 16)
            for j in range(n):
                mat[pl.ds(r, 16), 128 * j:128 * (j + 1)] = flat_ref[pl.ds(first + r * n + j, 16, stride=n), :].astype(BF16)
            return 0
        lax.fori_loop(0, height // 16, body, 0)
        cp = pltpu.make_async_copy(mat, out, osem.at[s])
        cp.start()
        copies.append(cp)
        first += height * n
    vec_ref[...] = flat_ref[first:first + vec_ref.shape[0], :]
    for i, rel in enumerate(plan):
        valid, src = source_of(rel, pos)
        for col in range(3):
            finish(3 * i + col, rel, col, valid, src)
    for cp in copies:
        cp.wait()


def gather(own, count, mats, vec_rows):
    rows = own.shape[0]
    devices = 2 * NA * NB * NX
    slot = (rows + 15) // 16 * 16
    parts = split_rows(slot, SHARE)
    vm = pl.BlockSpec(memory_space=pltpu.VMEM)
    outs = [jax.ShapeDtypeStruct(m, BF16) for m in mats] + [
        jax.ShapeDtypeStruct((vec_rows, 128), F32), jax.ShapeDtypeStruct((8, 128), F32)]
    return pl.pallas_call(
        functools.partial(gather_kernel, parts, rows, mats),
        out_shape=outs,
        in_specs=[vm, vm],
        out_specs=[pl.BlockSpec(memory_space=pl.ANY)] * len(mats) + [vm, vm],
        scratch_shapes=[
            pltpu.VMEM((devices, slot, 128), BF16), pltpu.VMEM((devices * rows, 128), F32),
            pltpu.SemaphoreType.DMA((84, 5)), pltpu.SemaphoreType.DMA((devices, 3)),
            pltpu.VMEM((11, 8, 128), F32), pltpu.SemaphoreType.DMA((5,)), pltpu.SemaphoreType.DMA((5,)),
            pltpu.SemaphoreType.DMA((len(mats),))] + [pltpu.VMEM(m, BF16) for m in mats],
        compiler_params=pltpu.CompilerParams(collective_id=0, has_side_effects=True, vmem_limit_bytes=67043328),
        name="gather_params",
    )(own, count)


def reduce_kernel(parts, rows, grad_ref, part_ref, out_ref, total_ref, part, rb_core, rb_x, rb_b, rb_a01, rb_a2, stage, acc,
                  ssem, send_c, recv_c, send_p, recv_x, recv_b, recv_a, tbuf, tsend, trecv):
    pos, core = coords()
    plan = list(reversed(steps()))
    depth = stage.shape[0]
    loads = []
    for rel in plan:
        loads.append((rel, 1))
        loads.append((rel, 0))

    def load(i):
        rel, other = loads[i]
        valid, src = source_of(rel, pos)
        o = flat(src, 1 - core if other else core)
        return valid, o, pltpu.make_async_copy(grad_ref.at[pl.ds(pl.multiple_of(o * rows, 8), rows), :], stage.at[i % depth, 0:rows, :], ssem.at[i % depth])

    def start_load(i):
        valid, o, cp = load(i)
        when(valid, cp.start)

    tbuf[0] = part_ref[...]
    for i in range(depth):
        start_load(i)
    if stage.shape[1] > rows:
        for i in range(depth):
            stage[i, rows:, :] = jnp.zeros((stage.shape[1] - rows, 128), F32)
    total = Total(pos, core, tbuf, tsend, trecv)
    greet(pos, core)
    hooks = total.hooks(6, 14)

    def core_copy(rel):
        valid, src = source_of(rel, pos)
        chip = flat(src, 0) // 2
        return valid, src, pltpu.make_async_remote_copy(
            src_ref=part.at[flat(src, 1 - core)], dst_ref=rb_core.at[chip], send_sem=send_c.at[chip], recv_sem=recv_c.at[chip],
            device_id=device(pos, 1 - core), device_id_type=MESH)

    def convert(i):
        rel, other = loads[i]
        valid, o, cp = load(i)

        def inner():
            cp.wait()
            def body(t, _):
                r = pl.multiple_of(t * 16, 16)
                part[o, pl.ds(r, 16), :] = stage[i % depth, pl.ds(r, 16), :].astype(BF16)
                return 0
            lax.fori_loop(0, part.shape[1] // 16, body, 0, unroll=False)
        when(valid, inner)

    def buffer(direction, src, col):
        lo, n = parts[col]
        if direction == 3:
            return rb_x.at[src[0] * NB + src[1], pl.ds(lo, n), :], recv_x.at[src[0] * NB + src[1], col]
        if direction == 2:
            return rb_b.at[src[0] * NX + src[2], pl.ds(lo, n), :], recv_b.at[src[0] * NX + src[2], col]
        chip = (src[0] * NB + src[1]) * NX + src[2]
        if col == 2:
            return rb_a2.at[direction, chip], recv_a.at[direction, chip, col]
        return rb_a01.at[direction, src[0], pl.ds(lo, n), :], recv_a.at[direction, chip, col]

    def parent_copy(rel, col, k, src):
        order = ORDERS[col]
        d = [d for d in order if rel[d] != 0][-1]
        to = list(pos)
        if d == 0:
            direction = 0 if rel[0] < 0 else 1
            to[0] = pos[0] - 1 if rel[0] < 0 else pos[0] + 1
        else:
            direction = 1 + d
            to[d] = 1 - pos[d]
        lo, n = parts[col]
        dst, sem = buffer(direction, src, col)
        return pltpu.make_async_remote_copy(
            src_ref=part.at[flat(src, core), pl.ds(lo, n), :], dst_ref=dst, send_sem=send_p.at[k], recv_sem=sem,
            device_id=device(to, core), device_id_type=MESH)

    def arrived(direction, src, col):
        dst, sem = buffer(direction, src, col)
        return pltpu.make_async_remote_copy(src_ref=dst, dst_ref=dst, send_sem=send_p.at[0], recv_sem=sem,
                                            device_id=device(pos, 1 - core), device_id_type=MESH)

    def combine(k, rel, col):
        valid, src = source_of(rel, pos)
        lo, n = parts[col]

        def inner():
            o = flat(src, core)
            chip = flat(src, 0) // 2
            if col == 0:
                core_copy(rel)[2].wait_recv()
            kids = children(rel, ORDERS[col], pos)
            sure = [d for c, _, d in kids if c is None]
            maybe = [(c, d) for c, _, d in kids if c is not None]
            for d in sure:
                arrived(d, src, col).wait_recv()
            refs = [buffer(d, src, col)[0] for d in sure]

            def fold(write):
                def body(t, _):
                    r = pl.multiple_of(t * 16, 16)
                    v = part[o, pl.ds(lo + r, 16), :].astype(F32) + rb_core[chip, pl.ds(lo + r, 16), :].astype(F32)
                    for ref in refs:
                        v = v + ref[pl.ds(r, 16), :].astype(F32)
                    write(r, v)
                    return 0
                lax.fori_loop(0, n // 16, body, 0)

            root = rel == (0, 0, 0)

            def emit(r, v):
                if root:
                    out_ref[pl.ds(lo + r, 16), :] = v
                else:
                    part[o, pl.ds(lo + r, 16), :] = v.astype(BF16)

            def to_acc(r, v):
                acc[pl.ds(r, 16), :] = v

            if not maybe:
                fold(emit)
            else:
                fold(to_acc)
                for c, d in maybe:
                    def add(d=d):
                        arrived(d, src, col).wait_recv()
                        ref = buffer(d, src, col)[0]
                        def body(t, _):
                            r = pl.multiple_of(t * 16, 16)
                            acc[pl.ds(r, 16), :] = acc[pl.ds(r, 16), :] + ref[pl.ds(r, 16), :].astype(F32)
                            return 0
                        lax.fori_loop(0, n // 16, body, 0)
                    when(c, add)
                def last(t, _):
                    r = pl.multiple_of(t * 16, 16)
                    emit(r, acc[pl.ds(r, 16), :])
                    return 0
                lax.fori_loop(0, n // 16, last, 0)
            if not root:
                parent_copy(rel, col, k, src).start()
        when(valid, inner)

    AHEAD = 2
    def prepare(j):
        for i in (2 * j, 2 * j + 1):
            convert(i)
            if i + depth < len(loads):
                start_load(i + depth)
            if i % 2 == 0:
                valid, src, cp = core_copy(plan[j])
                when(valid, cp.start)
    for j in range(AHEAD):
        prepare(j)
    for j in range(len(plan)):
        if j + AHEAD < len(plan):
            prepare(j + AHEAD)
        for col in range(3):
            combine(3 * j + col, plan[j], col)
            for h in hooks.get(3 * j + col, ()):
                h()
    total_ref[...] = tbuf[2 * total.n]
    for j, rel in enumerate(plan):
        valid, src, cp = core_copy(rel)
        when(valid, cp.wait_send)
        if rel != (0, 0, 0):
            for col in range(3):
                when(valid, parent_copy(rel, col, 3 * j + col, src).wait_send)


def reduce(grad, part, rows):
    devices = 2 * NA * NB * NX
    slot = (rows + 15) // 16 * 16
    parts = split_rows(slot, SHARE)
    two = parts[0][1] + parts[1][1]
    vm = pl.BlockSpec(memory_space=pltpu.VMEM)
    return pl.pallas_call(
        functools.partial(reduce_kernel, parts, rows),
        out_shape=[jax.ShapeDtypeStruct((slot, 128), F32), jax.ShapeDtypeStruct((8, 128), F32)],
        in_specs=[pl.BlockSpec(memory_space=pl.ANY), vm],
        out_specs=[vm, vm],
        scratch_shapes=[
            pltpu.VMEM((devices, slot, 128), BF16), pltpu.VMEM((devices // 2, slot, 128), BF16),
            pltpu.VMEM((NA * NB, slot, 128), BF16), pltpu.VMEM((NA * NX, slot, 128), BF16),
            pltpu.VMEM((2, NA, two, 128), BF16), pltpu.VMEM((2, devices // 2, parts[2][1], 128), BF16),
            pltpu.VMEM((4, slot, 128), F32), pltpu.VMEM((max(p[1] for p in parts), 128), F32),
            pltpu.SemaphoreType.DMA((4,)), pltpu.SemaphoreType.DMA((devices // 2,)), pltpu.SemaphoreType.DMA((devices // 2,)),
            pltpu.SemaphoreType.DMA((84,)), pltpu.SemaphoreType.DMA((NA * NB, 3)), pltpu.SemaphoreType.DMA((NA * NX, 3)),
            pltpu.SemaphoreType.DMA((2, devices // 2, 3)),
            pltpu.VMEM((11, 8, 128), F32), pltpu.SemaphoreType.DMA((5,)), pltpu.SemaphoreType.DMA((5,))],
        compiler_params=pltpu.CompilerParams(collective_id=1, has_side_effects=True, vmem_limit_bytes=67043328),
        name="reduce_gradient",
    )(grad, part)


norm_epsilon = 1e-06
adam_epsilon = 1e-08
beta_one = 0.9
beta_two = 0.999
learn_rate = 0.1
weight_decay = 0.05


def unpack(tiled):
    flat = tiled.reshape(-1)
    layout = [(D, 3 * D), (D, D), (D, FF), (D, FF)]
    pieces = []
    offset = 0
    for height, breadth in layout:
        pieces.append(flat[offset : offset + height * breadth].reshape(height, breadth))
        offset = offset + height * breadth
    for length in [D] * 8 + [FF]:
        pieces.append(flat[offset : offset + length].astype(jnp.float32))
        offset = offset + length
    return pieces


def layer_norm(values, gain, shift):
    center = values - jnp.mean(values, -1, keepdims=True)
    spread = jnp.mean(center * center, -1, keepdims=True)
    return center * lax.rsqrt(spread + norm_epsilon) * gain + shift


def exact_gelu(values):
    return jax.nn.gelu(values, approximate=False)


def collect(shard):
    lowered = shard.astype(jnp.bfloat16)
    whole = lax.all_gather(lowered, ("dp", "fsdp"), axis=0, tiled=True)
    return whole


def reduce_rows(full):
    summed = lax.psum_scatter(full, ("dp", "fsdp"), scatter_dimension=0, tiled=True)
    return summed


def gathered_weights(params, count, custom):
    mats = ((D, 3 * D), (D, D), (D, FF), (D, FF))
    if not custom:
        return unpack(collect(params)) + [lax.psum(count, ("dp", "fsdp"))]
    total_rows = params.shape[0] * 2 * NA * NB * NX
    used = sum(h * w for h, w in mats) // 128
    outs = gather(params, jnp.full((8, 128), count), mats, total_rows - used)
    pieces = list(outs[:4])
    flat_vectors = outs[4].reshape(-1)
    offset = 0
    for length in [D] * 8 + [FF]:
        pieces.append(flat_vectors[offset : offset + length])
        offset = offset + length
    return pieces + [outs[5][0, 0]]


def contract_rows(left, right):
    return lax.dot_general(
        left, right, (((0,), (0,)), ((), ())), preferred_element_type=jnp.float32
    )


def contract_cols(left, right):
    return lax.dot_general(
        left, right, (((1,), (1,)), ((), ())), preferred_element_type=jnp.float32
    )


def column_sum(values):
    return jnp.sum(values.astype(jnp.float32), 0)


def shards(custom, tokens, valid_mask, target, params, first_moment, second_moment):
    token_rows = tokens.shape[0]
    places = token_rows // FRAMES
    devices = lax.axis_size("dp") * lax.axis_size("fsdp")
    lane_count = params.shape[1]
    total_rows = params.shape[0] * devices
    score_scale = HEAD ** (-0.5)
    mask_values = valid_mask.astype(jnp.float32)
    pieces = gathered_weights(params, jnp.sum(mask_values), custom)
    kept_count = pieces[-1]
    (
        w_qkv,
        w_proj,
        w_in,
        w_out,
        gain_one,
        shift_one,
        bias_query,
        bias_value,
        bias_proj,
        gain_two,
        shift_two,
        bias_out,
        bias_in,
    ) = pieces[:-1]
    inputs = tokens.astype(jnp.float32)
    normed_low = layer_norm(inputs, gain_one, shift_one).astype(jnp.bfloat16)
    bias_all = jnp.concatenate([bias_query, jnp.zeros_like(bias_query), bias_value])
    mixed_low = (jnp.dot(normed_low, w_qkv, preferred_element_type=jnp.float32) + bias_all).astype(
        jnp.bfloat16
    )
    heads_view = mixed_low.reshape(places, FRAMES, 3, HEADS, HEAD)
    queries = heads_view[:, :, 0]
    key_part = heads_view[:, :, 1]
    values = heads_view[:, :, 2]
    scores = (
        jnp.einsum("pfhe,pghe->phfg", queries, key_part, preferred_element_type=jnp.float32)
        * score_scale
    )
    row_max = jnp.max(scores, -1, keepdims=True)
    log_total = row_max + jnp.log(jnp.sum(jnp.exp(scores - row_max), -1, keepdims=True))
    probs = jnp.exp(scores - log_total)
    probs_low = probs.astype(jnp.bfloat16)
    attended = jnp.einsum("phfg,pghe->pfhe", probs_low, values, preferred_element_type=jnp.float32)
    attended_low = attended.reshape(token_rows, D).astype(jnp.bfloat16)
    branch = jnp.dot(attended_low, w_proj, preferred_element_type=jnp.float32) + bias_proj
    middle = inputs + branch
    normed_two_low = layer_norm(middle, gain_two, shift_two).astype(jnp.bfloat16)
    hidden = jnp.dot(normed_two_low, w_in, preferred_element_type=jnp.float32) + bias_in
    active_low = exact_gelu(hidden).astype(jnp.bfloat16)
    second_branch = contract_cols(active_low, w_out) + bias_out
    output = middle + second_branch
    misfit = output - target.astype(jnp.float32)
    squares = jnp.sum(mask_values * jnp.sum(misfit * misfit, -1))
    denominator = kept_count * D
    grad_out = 2.0 / denominator * mask_values[:, None] * misfit
    grad_out_low = grad_out.astype(jnp.bfloat16)
    grad_bias_out = column_sum(grad_out_low)
    grad_w_out = contract_rows(grad_out_low, active_low)
    grad_active = jnp.dot(grad_out_low, w_out, preferred_element_type=jnp.float32)
    gelu_value, gelu_pull = jax.vjp(exact_gelu, hidden)
    grad_hidden_low = gelu_pull(grad_active)[0].astype(jnp.bfloat16)
    grad_bias_in = column_sum(grad_hidden_low)
    grad_w_in = contract_rows(normed_two_low, grad_hidden_low)
    grad_normed_two = contract_cols(grad_hidden_low, w_in)
    norm_value, second_pull = jax.vjp(layer_norm, middle, gain_two, shift_two)
    grad_middle_norm, grad_gain_two, grad_shift_two = second_pull(grad_normed_two)
    grad_middle = grad_out + grad_middle_norm
    grad_branch_low = grad_middle.astype(jnp.bfloat16)
    grad_bias_proj = column_sum(grad_branch_low)
    grad_w_proj = contract_rows(attended_low, grad_branch_low)
    grad_attended_low = (
        contract_cols(grad_branch_low, w_proj)
        .astype(jnp.bfloat16)
        .reshape(places, FRAMES, HEADS, HEAD)
    )
    grad_values = jnp.einsum(
        "phfg,pfhe->pghe", probs_low, grad_attended_low, preferred_element_type=jnp.float32
    )
    grad_probs = jnp.einsum(
        "pfhe,pghe->phfg", grad_attended_low, values, preferred_element_type=jnp.float32
    )
    grad_scores_low = (
        probs * (grad_probs - jnp.sum(probs * grad_probs, -1, keepdims=True))
    ).astype(jnp.bfloat16)
    grad_queries = (
        jnp.einsum("phfg,pghe->pfhe", grad_scores_low, key_part, preferred_element_type=jnp.float32)
        * score_scale
    )
    grad_keys = (
        jnp.einsum("phfg,pfhe->pghe", grad_scores_low, queries, preferred_element_type=jnp.float32)
        * score_scale
    )
    grad_mixed_low = (
        jnp.stack([grad_queries, grad_keys, grad_values], 2)
        .reshape(token_rows, 3 * D)
        .astype(jnp.bfloat16)
    )
    grad_bias_query = column_sum(grad_mixed_low[:, :D])
    grad_bias_value = column_sum(grad_mixed_low[:, 2 * D :])
    grad_w_qkv = contract_rows(normed_low, grad_mixed_low)
    grad_normed_one = contract_cols(grad_mixed_low, w_qkv)
    first_value, first_pull = jax.vjp(layer_norm, inputs, gain_one, shift_one)
    grad_inputs_norm, grad_gain_one, grad_shift_one = first_pull(grad_normed_one)
    grad_inputs = grad_middle + grad_inputs_norm
    used_grad = jnp.concatenate(
        [
            grad_w_qkv.reshape(-1),
            grad_w_proj.reshape(-1),
            grad_w_in.reshape(-1),
            grad_w_out.reshape(-1),
            grad_gain_one,
            grad_shift_one,
            grad_bias_query,
            grad_bias_value,
            grad_bias_proj,
            grad_gain_two,
            grad_shift_two,
            grad_bias_out,
            grad_bias_in,
        ]
    )
    padding = jnp.zeros((total_rows * lane_count - used_grad.shape[0],), jnp.float32)
    whole_grad = jnp.concatenate([used_grad, padding]).reshape(total_rows, lane_count)
    if custom:
        gradient, totals = reduce(whole_grad, jnp.full((8, 128), squares), params.shape[0])
        gradient, total_error = gradient[: params.shape[0]], totals[0, 0]
    else:
        gradient, total_error = reduce_rows(whole_grad), lax.psum(squares, ("dp", "fsdp"))
    loss = total_error / denominator
    new_first = beta_one * first_moment + (1.0 - beta_one) * gradient
    new_second = beta_two * second_moment + (1.0 - beta_two) * gradient * gradient
    first_hat = new_first / (1.0 - beta_one**STEP)
    second_hat = new_second / (1.0 - beta_two**STEP)
    new_params = params - learn_rate * (
        first_hat / (jnp.sqrt(second_hat) + adam_epsilon) + weight_decay * params
    )
    input_grad = grad_inputs * float(token_rows * devices * D)
    return (output.astype(jnp.bfloat16), loss, input_grad, new_params, new_first, new_second)


def solution(mesh):
    custom = mesh.shape["dp"] == NA * NB and mesh.shape["fsdp"] == 2 * NX
    return jax.shard_map(
        functools.partial(shards, custom),
        mesh=mesh,
        in_specs=(
            P(("dp", "fsdp"), None),
            P(("dp", "fsdp")),
            P(("dp", "fsdp"), None),
            P(("dp", "fsdp"), None),
            P(("dp", "fsdp"), None),
            P(("dp", "fsdp"), None),
        ),
        out_specs=(
            P(("dp", "fsdp"), None),
            P(),
            P(("dp", "fsdp"), None),
            P(("dp", "fsdp"), None),
            P(("dp", "fsdp"), None),
            P(("dp", "fsdp"), None),
        ),
        check_vma=False,
    )
```

```python
import functools
import math

import jax
import jax.numpy as jnp
from jax import lax
from jax.experimental import pallas as pl
from jax.experimental.pallas import tpu as pltpu
from jax.sharding import PartitionSpec as P

D = 768
HEADS = 12
HEAD = 64
FF = 3072
FRAMES = 16
STEP = 10


norm_epsilon = 1e-06
adam_epsilon = 1e-08
beta_one = 0.9
beta_two = 0.999
learn_rate = 0.1
weight_decay = 0.05

def unpack(tiled):
    flat = tiled.reshape(-1)
    layout = [(D, 3 * D), (D, D), (D, FF), (D, FF)]
    pieces = []
    offset = 0
    for height, breadth in layout:
        pieces.append(flat[offset : offset + height * breadth].reshape(height, breadth))
        offset = offset + height * breadth
    for length in [D] * 8 + [FF]:
        pieces.append(flat[offset : offset + length].astype(jnp.float32))
        offset = offset + length
    return pieces


def collect(shard):
    lowered = shard.astype(jnp.bfloat16)
    whole = lax.all_gather(lowered, ("dp", "fsdp"), axis=0, tiled=True)
    return whole


def reduce_rows(full):
    summed = lax.psum_scatter(full, ("dp", "fsdp"), scatter_dimension=0, tiled=True)
    return summed


MESH = pl.DeviceIdType.MESH
NA, NB, NX = 4, 2, 2
ORDERS = ((0, 1, 2), (0, 2, 1), (1, 2, 0))


def coords():
    dp = lax.axis_index("dp")
    fs = lax.axis_index("fsdp")
    return (dp // NB, dp % NB, fs // 2), fs % 2


def device(pos, core):
    return (pos[0] * NB + pos[1], pos[2] * 2 + core)


def flat(pos, core):
    return ((pos[0] * NB + pos[1]) * NX + pos[2]) * 2 + core


def steps():
    out = []
    for da in range(-(NA - 1), NA):
        for db in range(2):
            for dx in range(2):
                out.append((abs(da) + db + dx, (da, db, dx)))
    out.sort(key=lambda t: t[0])
    return [r for _, r in out]


def children(rel, order, pos):
    last = -1
    for i, d in enumerate(order):
        if rel[d] != 0:
            last = i
    res = []

    def line(up):
        a = pos[0]
        if up:
            return (a + 1 < NA, (a + 1, pos[1], pos[2]), 0)
        return (a - 1 >= 0, (a - 1, pos[1], pos[2]), 1)

    def flip(d):
        p = list(pos)
        p[d] = 1 - p[d]
        return (None, tuple(p), 1 + d)

    if last >= 0 and order[last] == 0:
        res.append(line(rel[0] < 0))
    for i in range(last + 1, 3):
        d = order[i]
        if d == 0:
            res.append(line(True))
            res.append(line(False))
        else:
            res.append(flip(d))
    return res


def source_of(rel, pos):
    a = pos[0] + rel[0]
    valid = None
    if rel[0] > 0:
        valid = a < NA
    if rel[0] < 0:
        valid = a >= 0
    return valid, (a, (pos[1] + rel[1]) % 2, (pos[2] + rel[2]) % 2)


def when(cond, fn):
    if cond is None:
        fn()
    else:
        pl.when(cond)(fn)


def both(a, b):
    if a is None:
        return b
    if b is None:
        return a
    return jnp.logical_and(a, b)


def split_rows(rows, shares):
    tiles = rows // 16
    first = int(round(tiles * shares))
    return ((0, first * 16), (first * 16, first * 16), (2 * first * 16, rows - 2 * first * 16))


F32, BF16 = jnp.float32, jnp.bfloat16
SHARE = 0.389


def greet(pos, core):
    sem = pltpu.get_barrier_semaphore()
    a, b, x = pos
    fixed = [device(pos, 1 - core), device((a, 1 - b, x), core), device((a, b, 1 - x), core),
             device(((a + 2) % NA, b, x), core)]
    for d in fixed:
        pl.semaphore_signal(sem, inc=1, device_id=d, device_id_type=MESH)
    up, down = a + 1 < NA, a - 1 >= 0
    when(up, lambda: pl.semaphore_signal(sem, inc=1, device_id=device((a + 1, b, x), core), device_id_type=MESH))
    when(down, lambda: pl.semaphore_signal(sem, inc=1, device_id=device((a - 1, b, x), core), device_id_type=MESH))
    pl.semaphore_wait(sem, len(fixed) + up.astype(jnp.int32) + down.astype(jnp.int32))


class Total:
    def __init__(self, pos, core, buf, send, recv):
        a, b, x = pos
        flip = a + 1 - 2 * (a % 2)
        partners = [device(pos, 1 - core), device((a, b, 1 - x), core), device((a, 1 - b, x), core),
                    device((flip, b, x), core), device(((a + 2) % NA, b, x), core)]
        self.buf = buf
        self.copies = [pltpu.make_async_remote_copy(
            src_ref=buf.at[2 * i], dst_ref=buf.at[2 * i + 1], send_sem=send.at[i], recv_sem=recv.at[i],
            device_id=p, device_id_type=MESH) for i, p in enumerate(partners)]
        self.n = len(partners)

    def start(self, i):
        self.copies[i].start()

    def end(self, i):
        self.copies[i].wait()
        self.buf[2 * i + 2] = self.buf[2 * i] + self.buf[2 * i + 1]

    def hooks(self, first, gap):
        table = {}
        for i in range(self.n):
            table.setdefault(first + i * gap, []).append(functools.partial(self.start, i))
            table.setdefault(first + i * gap + gap - 2, []).append(functools.partial(self.end, i))
        return table


def gather_kernel(parts, rows, mats, own_ref, count_ref, *refs):
    nm = len(mats)
    outs, vec_ref, total_ref = refs[:nm], refs[nm], refs[nm + 1]
    slots, flat_ref, send, recv, tbuf, tsend, trecv, osem = refs[nm + 2:nm + 10]
    mat_refs = refs[nm + 10:]
    pos, core = coords()
    me = flat(pos, core)
    slots[me, 0:rows, :] = own_ref[...].astype(BF16)
    if slots.shape[1] > rows:
        slots[me, rows:, :] = jnp.zeros((slots.shape[1] - rows, 128), BF16)
    tbuf[0] = count_ref[...]
    total = Total(pos, core, tbuf, tsend, trecv)
    greet(pos, core)
    hooks = total.hooks(6, 14)
    plan = steps()
    order_k = []
    for rel in plan:
        for col in range(3):
            order_k.append((rel, col))

    def chunk(idx, col):
        lo, n = parts[col]
        return slots.at[idx, pl.ds(lo, n), :]

    def copy(idx, col, k, direction, to):
        return pltpu.make_async_remote_copy(
            src_ref=chunk(idx, col), dst_ref=chunk(idx, col),
            send_sem=send.at[k, direction], recv_sem=recv.at[idx, col],
            device_id=to, device_id_type=MESH)

    def widen(idx):
        base = pl.multiple_of(idx * rows, 8)
        def body(i, _):
            r = pl.multiple_of(i * 112, 16)
            flat_ref[pl.ds(pl.multiple_of(base + r, 8), 112), :] = slots[idx, pl.ds(r, 112), :].astype(F32)
            return 0
        lax.fori_loop(0, rows // 112, body, 0)
        rest = rows % 112
        if rest:
            r = rows // 112 * 112
            flat_ref[pl.ds(pl.multiple_of(base + r, 8), rest), :] = slots[idx, r:r + rest, :].astype(F32)

    def run(k, rel, col, valid, src):
        def inner():
            idx = flat(src, core)
            if rel != (0, 0, 0):
                copy(idx, col, k, 0, device(pos, 1 - core)).wait_recv()
            for cond, child, direction in children(rel, ORDERS[col], pos):
                when(cond, lambda child=child, direction=direction: copy(idx, col, k, direction, device(child, core)).start())
            copy(idx, col, k, 4, device(pos, 1 - core)).start()
        when(valid, inner)

    def sibling(rel, k0):
        valid, src = source_of(rel, pos)
        def inner():
            other = flat(src, 1 - core)
            for col in range(3):
                copy(other, col, k0 + col, 4, device(pos, 1 - core)).wait_recv()
            widen(flat(src, core))
            widen(other)
        when(valid, inner)

    def finish(k, rel, col, valid, src):
        def inner():
            idx = flat(src, core)
            for cond, child, direction in children(rel, ORDERS[col], pos):
                when(cond, lambda child=child, direction=direction: copy(idx, col, k, direction, device(child, core)).wait_send())
            copy(idx, col, k, 4, device(pos, 1 - core)).wait_send()
        when(valid, inner)

    LAG = 2
    for i, rel in enumerate(plan):
        valid, src = source_of(rel, pos)
        for col in range(3):
            k = 3 * i + col
            run(k, rel, col, valid, src)
            for h in hooks.get(k, ()):
                h()
        if i >= LAG:
            sibling(plan[i - LAG], 3 * (i - LAG))
    for i in range(len(plan) - LAG, len(plan)):
        sibling(plan[i], 3 * i)
    total_ref[...] = tbuf[2 * total.n]
    first = 0
    copies = []
    for (height, width), mat, out, s in zip(mats, mat_refs, outs, range(nm)):
        n = width // 128
        def body(i, _, mat=mat, n=n, first=first):
            r = pl.multiple_of(i * 16, 16)
            for j in range(n):
                mat[pl.ds(r, 16), 128 * j:128 * (j + 1)] = flat_ref[pl.ds(first + r * n + j, 16, stride=n), :].astype(BF16)
            return 0
        lax.fori_loop(0, height // 16, body, 0)
        cp = pltpu.make_async_copy(mat, out, osem.at[s])
        cp.start()
        copies.append(cp)
        first += height * n
    vec_ref[...] = flat_ref[first:first + vec_ref.shape[0], :]
    for i, rel in enumerate(plan):
        valid, src = source_of(rel, pos)
        for col in range(3):
            finish(3 * i + col, rel, col, valid, src)
    for cp in copies:
        cp.wait()


def gather(own, count, mats, vec_rows):
    rows = own.shape[0]
    devices = 2 * NA * NB * NX
    slot = (rows + 15) // 16 * 16
    parts = split_rows(slot, SHARE)
    vm = pl.BlockSpec(memory_space=pltpu.VMEM)
    outs = [jax.ShapeDtypeStruct(m, BF16) for m in mats] + [
        jax.ShapeDtypeStruct((vec_rows, 128), F32), jax.ShapeDtypeStruct((8, 128), F32)]
    return pl.pallas_call(
        functools.partial(gather_kernel, parts, rows, mats),
        out_shape=outs,
        in_specs=[vm, vm],
        out_specs=[pl.BlockSpec(memory_space=pl.ANY)] * len(mats) + [vm, vm],
        scratch_shapes=[
            pltpu.VMEM((devices, slot, 128), BF16), pltpu.VMEM((devices * rows, 128), F32),
            pltpu.SemaphoreType.DMA((84, 5)), pltpu.SemaphoreType.DMA((devices, 3)),
            pltpu.VMEM((11, 8, 128), F32), pltpu.SemaphoreType.DMA((5,)), pltpu.SemaphoreType.DMA((5,)),
            pltpu.SemaphoreType.DMA((len(mats),))] + [pltpu.VMEM(m, BF16) for m in mats],
        compiler_params=pltpu.CompilerParams(collective_id=0, has_side_effects=True, vmem_limit_bytes=67043328),
        name="gather_params",
    )(own, count)


def reduce_kernel(parts, rows, grad_ref, part_ref, out_ref, total_ref, part, rb_core, rb_x, rb_b, rb_a01, rb_a2, stage, acc,
                  ssem, send_c, recv_c, send_p, recv_x, recv_b, recv_a, tbuf, tsend, trecv):
    pos, core = coords()
    plan = list(reversed(steps()))
    depth = stage.shape[0]
    loads = []
    for rel in plan:
        loads.append((rel, 1))
        loads.append((rel, 0))

    def load(i):
        rel, other = loads[i]
        valid, src = source_of(rel, pos)
        o = flat(src, 1 - core if other else core)
        return valid, o, pltpu.make_async_copy(grad_ref.at[pl.ds(pl.multiple_of(o * rows, 8), rows), :], stage.at[i % depth, 0:rows, :], ssem.at[i % depth])

    def start_load(i):
        valid, o, cp = load(i)
        when(valid, cp.start)

    tbuf[0] = part_ref[...]
    for i in range(depth):
        start_load(i)
    if stage.shape[1] > rows:
        for i in range(depth):
            stage[i, rows:, :] = jnp.zeros((stage.shape[1] - rows, 128), F32)
    total = Total(pos, core, tbuf, tsend, trecv)
    greet(pos, core)
    hooks = total.hooks(6, 14)

    def core_copy(rel):
        valid, src = source_of(rel, pos)
        chip = flat(src, 0) // 2
        return valid, src, pltpu.make_async_remote_copy(
            src_ref=part.at[flat(src, 1 - core)], dst_ref=rb_core.at[chip], send_sem=send_c.at[chip], recv_sem=recv_c.at[chip],
            device_id=device(pos, 1 - core), device_id_type=MESH)

    def convert(i):
        rel, other = loads[i]
        valid, o, cp = load(i)

        def inner():
            cp.wait()
            def body(t, _):
                r = pl.multiple_of(t * 16, 16)
                part[o, pl.ds(r, 16), :] = stage[i % depth, pl.ds(r, 16), :].astype(BF16)
                return 0
            lax.fori_loop(0, part.shape[1] // 16, body, 0, unroll=False)
        when(valid, inner)

    def buffer(direction, src, col):
        lo, n = parts[col]
        if direction == 3:
            return rb_x.at[src[0] * NB + src[1], pl.ds(lo, n), :], recv_x.at[src[0] * NB + src[1], col]
        if direction == 2:
            return rb_b.at[src[0] * NX + src[2], pl.ds(lo, n), :], recv_b.at[src[0] * NX + src[2], col]
        chip = (src[0] * NB + src[1]) * NX + src[2]
        if col == 2:
            return rb_a2.at[direction, chip], recv_a.at[direction, chip, col]
        return rb_a01.at[direction, src[0], pl.ds(lo, n), :], recv_a.at[direction, chip, col]

    def parent_copy(rel, col, k, src):
        order = ORDERS[col]
        d = [d for d in order if rel[d] != 0][-1]
        to = list(pos)
        if d == 0:
            direction = 0 if rel[0] < 0 else 1
            to[0] = pos[0] - 1 if rel[0] < 0 else pos[0] + 1
        else:
            direction = 1 + d
            to[d] = 1 - pos[d]
        lo, n = parts[col]
        dst, sem = buffer(direction, src, col)
        return pltpu.make_async_remote_copy(
            src_ref=part.at[flat(src, core), pl.ds(lo, n), :], dst_ref=dst, send_sem=send_p.at[k], recv_sem=sem,
            device_id=device(to, core), device_id_type=MESH)

    def arrived(direction, src, col):
        dst, sem = buffer(direction, src, col)
        return pltpu.make_async_remote_copy(src_ref=dst, dst_ref=dst, send_sem=send_p.at[0], recv_sem=sem,
                                            device_id=device(pos, 1 - core), device_id_type=MESH)

    def combine(k, rel, col):
        valid, src = source_of(rel, pos)
        lo, n = parts[col]

        def inner():
            o = flat(src, core)
            chip = flat(src, 0) // 2
            if col == 0:
                core_copy(rel)[2].wait_recv()
            kids = children(rel, ORDERS[col], pos)
            sure = [d for c, _, d in kids if c is None]
            maybe = [(c, d) for c, _, d in kids if c is not None]
            for d in sure:
                arrived(d, src, col).wait_recv()
            refs = [buffer(d, src, col)[0] for d in sure]

            def fold(write):
                def body(t, _):
                    r = pl.multiple_of(t * 16, 16)
                    v = part[o, pl.ds(lo + r, 16), :].astype(F32) + rb_core[chip, pl.ds(lo + r, 16), :].astype(F32)
                    for ref in refs:
                        v = v + ref[pl.ds(r, 16), :].astype(F32)
                    write(r, v)
                    return 0
                lax.fori_loop(0, n // 16, body, 0)

            root = rel == (0, 0, 0)

            def emit(r, v):
                if root:
                    out_ref[pl.ds(lo + r, 16), :] = v
                else:
                    part[o, pl.ds(lo + r, 16), :] = v.astype(BF16)

            def to_acc(r, v):
                acc[pl.ds(r, 16), :] = v

            if not maybe:
                fold(emit)
            else:
                fold(to_acc)
                for c, d in maybe:
                    def add(d=d):
                        arrived(d, src, col).wait_recv()
                        ref = buffer(d, src, col)[0]
                        def body(t, _):
                            r = pl.multiple_of(t * 16, 16)
                            acc[pl.ds(r, 16), :] = acc[pl.ds(r, 16), :] + ref[pl.ds(r, 16), :].astype(F32)
                            return 0
                        lax.fori_loop(0, n // 16, body, 0)
                    when(c, add)
                def last(t, _):
                    r = pl.multiple_of(t * 16, 16)
                    emit(r, acc[pl.ds(r, 16), :])
                    return 0
                lax.fori_loop(0, n // 16, last, 0)
            if not root:
                parent_copy(rel, col, k, src).start()
        when(valid, inner)

    AHEAD = 2
    def prepare(j):
        for i in (2 * j, 2 * j + 1):
            convert(i)
            if i + depth < len(loads):
                start_load(i + depth)
            if i % 2 == 0:
                valid, src, cp = core_copy(plan[j])
                when(valid, cp.start)
    for j in range(AHEAD):
        prepare(j)
    for j in range(len(plan)):
        if j + AHEAD < len(plan):
            prepare(j + AHEAD)
        for col in range(3):
            combine(3 * j + col, plan[j], col)
            for h in hooks.get(3 * j + col, ()):
                h()
    total_ref[...] = tbuf[2 * total.n]
    for j, rel in enumerate(plan):
        valid, src, cp = core_copy(rel)
        when(valid, cp.wait_send)
        if rel != (0, 0, 0):
            for col in range(3):
                when(valid, parent_copy(rel, col, 3 * j + col, src).wait_send)


def reduce(grad, part, rows):
    devices = 2 * NA * NB * NX
    slot = (rows + 15) // 16 * 16
    parts = split_rows(slot, SHARE)
    two = parts[0][1] + parts[1][1]
    vm = pl.BlockSpec(memory_space=pltpu.VMEM)
    return pl.pallas_call(
        functools.partial(reduce_kernel, parts, rows),
        out_shape=[jax.ShapeDtypeStruct((slot, 128), F32), jax.ShapeDtypeStruct((8, 128), F32)],
        in_specs=[pl.BlockSpec(memory_space=pl.ANY), vm],
        out_specs=[vm, vm],
        scratch_shapes=[
            pltpu.VMEM((devices, slot, 128), BF16), pltpu.VMEM((devices // 2, slot, 128), BF16),
            pltpu.VMEM((NA * NB, slot, 128), BF16), pltpu.VMEM((NA * NX, slot, 128), BF16),
            pltpu.VMEM((2, NA, two, 128), BF16), pltpu.VMEM((2, devices // 2, parts[2][1], 128), BF16),
            pltpu.VMEM((4, slot, 128), F32), pltpu.VMEM((max(p[1] for p in parts), 128), F32),
            pltpu.SemaphoreType.DMA((4,)), pltpu.SemaphoreType.DMA((devices // 2,)), pltpu.SemaphoreType.DMA((devices // 2,)),
            pltpu.SemaphoreType.DMA((84,)), pltpu.SemaphoreType.DMA((NA * NB, 3)), pltpu.SemaphoreType.DMA((NA * NX, 3)),
            pltpu.SemaphoreType.DMA((2, devices // 2, 3)),
            pltpu.VMEM((11, 8, 128), F32), pltpu.SemaphoreType.DMA((5,)), pltpu.SemaphoreType.DMA((5,))],
        compiler_params=pltpu.CompilerParams(collective_id=1, has_side_effects=True, vmem_limit_bytes=67043328),
        name="reduce_gradient",
    )(grad, part)


ERF_TOP = (0.00022905065861350646, 0.0034082910107109506, 0.050955695062380861, 0.18520832239976145, 1.128379143519084)
ERF_LOW = (-1.1791602954361697e-7, 0.000023547966471313185, 0.0010179625278914885, 0.014070470171167667,
           0.11098505178285362, 0.49746925110067538, 1.0)


def erf(v):
    v = jnp.clip(v, -3.832506856900711, 3.832506856900711)
    s = v * v
    top = ERF_TOP[0]
    for c in ERF_TOP[1:]:
        top = top * s + c
    low = ERF_LOW[0]
    for c in ERF_LOW[1:]:
        low = low * s + c
    return v * top / low


def dot(a, b):
    return jnp.dot(a, b, preferred_element_type=F32)


def dot_nt(a, b):
    return lax.dot_general(a, b, (((1,), (1,)), ((), ())), preferred_element_type=F32)


def dot_tn(a, b):
    return lax.dot_general(a, b, (((0,), (0,)), ((), ())), preferred_element_type=F32)


def loop(n, body):
    def step(i, carry):
        body(i)
        return carry
    lax.fori_loop(0, n, step, 0)


def at(i, size):
    return pl.ds(pl.multiple_of(i * size, size), size)


def compute_kernel(rows_total, x_ref, target_ref, mask_ref, vec_ref, count_ref, wq_hbm, wp_hbm, wi_hbm, wo_hbm,
                   act_ref, igrad_ref, sq_ref, grad_hbm,
                   wq, wp, wi, wo, mixed, probs, att, middle, slope, active, left, gout, glow, ghid, gmix, stage, vstage, wsem, ssem):
    tokens = x_ref.shape[0]
    scale = HEAD ** (-0.5)
    loads = [pltpu.make_async_copy(h, w, wsem.at[i]) for i, (h, w) in enumerate(
        ((wq_hbm, wq), (wp_hbm, wp), (wi_hbm, wi), (wo_hbm, wo)))]
    for c in loads:
        c.start()
    used_rows = (3 * D * D + D * D + 2 * D * FF) // 128

    def vector(row, n):
        return jnp.concatenate([vec_ref[row + j:row + j + 1, :] for j in range(n)], axis=1)

    per = D // 128
    gain_one, shift_one, bias_query, bias_value, bias_proj, gain_two, shift_two, bias_out = [
        vector(per * i, per) for i in range(8)]
    bias_in_row = 8 * per
    vstage[...] = jnp.zeros_like(vstage)

    def put_vector(i, v):
        for j in range(v.shape[1] // 128):
            vstage[per * i + j:per * i + j + 1, :] = v[:, 128 * j:128 * (j + 1)]

    def stats(v):
        mean = jnp.mean(v, -1, keepdims=True)
        center = v - mean
        r = lax.rsqrt(jnp.mean(center * center, -1, keepdims=True) + norm_epsilon)
        return center * r, r

    RB = 128
    nrb = tokens // RB
    low = glow

    def flip(dst):
        def body(i):
            left[dst, at(i, 128), :] = low[:, at(i, 128)].T
        loop(D // 128, body)

    def ln_one(i):
        z, _ = stats(x_ref[at(i, RB), :].astype(F32))
        low[at(i, RB), :] = (z * gain_one + shift_one).astype(BF16)
    loop(nrb, ln_one)
    loads[0].wait()
    BN = 256

    def qkv(part, bias):
        def body(i):
            j = i + part * (D // BN)
            v = dot(low[...], wq[:, at(j, BN)])
            if bias is not None:
                v = v + vec_bias[0:1, at(i, BN)]
            mixed[:, at(j, BN)] = v.astype(BF16)
        loop(D // BN, body)
    vec_bias = middle
    middle[0:1, :] = bias_query
    qkv(0, True)
    qkv(1, None)
    middle[0:1, :] = bias_value
    qkv(2, True)
    flip(0)

    pairs = HEADS // 2
    lane = lax.broadcasted_iota(jnp.int32, (128, 128), 1)
    lower = lane < HEAD
    r256 = lax.broadcasted_iota(jnp.int32, (128, 256), 0) // FRAMES
    c256 = (lax.broadcasted_iota(jnp.int32, (128, 256), 1) % 128) // FRAMES
    same = r256 == c256

    def stack(v):
        zero = jnp.zeros_like(v)
        return jnp.concatenate([jnp.where(lower, v, zero), jnp.where(lower, zero, v)], axis=0)

    def tile(i):
        g, p = i // pairs, i % pairs
        rows = at(g, 128)
        return rows, p

    def attention(i):
        rows, p = tile(i)
        q = mixed[rows, at(p, 128)]
        k = mixed[rows, at(p + pairs, 128)]
        v = mixed[rows, at(p + 2 * pairs, 128)]
        s = dot_nt(q, stack(k)) * scale
        s = jnp.where(same, s, -1e30)
        out = []
        for h in range(2):
            sh = s[:, 128 * h:128 * (h + 1)]
            e = jnp.exp(sh - jnp.max(sh, -1, keepdims=True))
            out.append(e / jnp.sum(e, -1, keepdims=True))
        pr = jnp.concatenate(out, axis=1)
        probs[i] = pr
        att[rows, at(p, 128)] = dot(pr.astype(BF16), stack(v)).astype(BF16)
    loop(pairs * (tokens // 128), attention)

    loads[1].wait()

    def project(i):
        v = dot(att[at(i, RB), :], wp[...])
        m = x_ref[at(i, RB), :].astype(F32) + (v + bias_proj)
        middle[at(i, RB), :] = m
        z, _ = stats(m)
        low[at(i, RB), :] = (z * gain_two + shift_two).astype(BF16)
    loop(nrb, project)
    loads[2].wait()

    def hidden(i):
        bias = jnp.concatenate([vec_ref[pl.ds(bias_in_row + 2 * i + j, 1), :] for j in range(BN // 128)], axis=1)
        h = dot(low[...], wi[:, at(i, BN)]) + bias
        cdf = 0.5 * (1.0 + erf(h * (0.5 ** 0.5)))
        pdf = jnp.exp(-0.5 * h * h) * (1.0 / math.sqrt(2.0 * math.pi))
        active[:, at(i, BN)] = (h * cdf).astype(BF16)
        slope[:, at(i, BN)] = cdf + h * pdf
    loop(FF // BN, hidden)
    flip(2)
    loads[3].wait()

    def second(i):
        gout[:, at(i, BN)] = dot_nt(active[...], wo[at(i, BN), :])
    loop(D // BN, second)
    factor = 2.0 / (count_ref[0:1, 0:1] * D)
    sq_ref[...] = jnp.zeros_like(sq_ref)

    def finish(i):
        o = middle[at(i, RB), :] + (gout[at(i, RB), :] + bias_out)
        act_ref[at(i, RB), :] = o.astype(BF16)
        misfit = o - target_ref[at(i, RB), :].astype(F32)
        m = mask_ref[at(i, RB), :]
        sq_ref[...] += jnp.full(sq_ref.shape, jnp.sum(m * jnp.sum(misfit * misfit, -1, keepdims=True)))
        g = (factor * m) * misfit
        gout[at(i, RB), :] = g
        low[at(i, RB), :] = g.astype(BF16)
    loop(nrb, finish)
    flip(3)

    def colsum(ref):
        return jnp.sum(ref.astype(F32), 0, keepdims=True)

    put_vector(7, colsum(low[...]))

    sent = []

    def weight_grad(lhs, rhs, width, first):
        n = width // 128
        half = D // 2
        for h in range(2):
            slot = len(sent) % 2
            if len(sent) >= 2:
                sent[-2].wait()
            size = half * n

            def body(j):
                v = dot(left[lhs, h * half:(h + 1) * half, :], rhs[:, at(j, BN)])
                for t in range(BN // 128):
                    stage[slot, pl.ds(2 * j + t, half, stride=n), :] = v[:, 128 * t:128 * (t + 1)]
            loop(width // BN, body)
            cp = pltpu.make_async_copy(stage.at[slot, 0:size, :], grad_hbm.at[first + h * size:first + (h + 1) * size, :], ssem.at[slot])
            cp.start()
            sent.append(cp)

    row_proj = 3 * D * D // 128
    row_in = row_proj + D * D // 128
    row_out = row_in + D * FF // 128
    weight_grad(3, active, FF, row_out)

    def back_hidden(i):
        v = dot(low[...], wo[:, at(i, BN)]) * slope[:, at(i, BN)]
        b = v.astype(BF16)
        ghid[:, at(i, BN)] = b
        s = jnp.sum(b.astype(F32), 0, keepdims=True)
        for t in range(BN // 128):
            vstage[pl.ds(bias_in_row + 2 * i + t, 1), :] = s[:, 128 * t:128 * (t + 1)]
    loop(FF // BN, back_hidden)
    weight_grad(2, ghid, FF, row_in)

    dnorm = igrad_ref

    def back_in(i):
        dnorm[:, at(i, BN)] = dot_nt(ghid[...], wi[at(i, BN), :])
    loop(D // BN, back_in)

    def norm_back(values, gain, dy):
        z, r = stats(values)
        dz = dy * gain
        m1 = jnp.mean(dz, -1, keepdims=True)
        m2 = jnp.mean(dz * z, -1, keepdims=True)
        return r * (dz - m1 - z * m2), jnp.sum(dy * z, 0, keepdims=True), jnp.sum(dy, 0, keepdims=True)

    zero = jnp.zeros((1, D), F32)

    def ln_two_back(i, carry):
        a, b, c = carry
        d, dg, ds = norm_back(middle[at(i, RB), :], gain_two, dnorm[at(i, RB), :])
        g = gout[at(i, RB), :] + d
        gout[at(i, RB), :] = g
        gl = g.astype(BF16)
        low[at(i, RB), :] = gl
        return a + dg, b + ds, c + jnp.sum(gl.astype(F32), 0, keepdims=True)
    a, b, c = lax.fori_loop(0, nrb, ln_two_back, (zero, zero, zero))
    put_vector(5, a)
    put_vector(6, b)
    put_vector(4, c)

    def flip_att(i):
        left[1, at(i, 128), :] = att[:, at(i, 128)].T
    loop(D // 128, flip_att)
    weight_grad(1, low, D, row_proj)

    def back_proj(i):
        att[:, at(i, BN)] = dot_nt(low[...], wp[at(i, BN), :]).astype(BF16)
    loop(D // BN, back_proj)

    def attention_back(i):
        rows, p = tile(i)
        q = mixed[rows, at(p, 128)]
        k = mixed[rows, at(p + pairs, 128)]
        v = mixed[rows, at(p + 2 * pairs, 128)]
        do = att[rows, at(p, 128)]
        pr = probs[i]
        dp = dot_nt(do, stack(v))
        out = []
        for h in range(2):
            ph, dh = pr[:, 128 * h:128 * (h + 1)], dp[:, 128 * h:128 * (h + 1)]
            out.append((ph * (dh - jnp.sum(ph * dh, -1, keepdims=True))).astype(BF16))
        gmix[rows, at(p, 128)] = (dot(jnp.concatenate(out, axis=1), stack(k)) * scale).astype(BF16)
        gmix[rows, at(p + pairs, 128)] = (dot_tn(jnp.concatenate(out, axis=0), stack(q)) * scale).astype(BF16)
        pl_low = jnp.concatenate([pr[:, :128], pr[:, 128:]], axis=0).astype(BF16)
        gmix[rows, at(p + 2 * pairs, 128)] = dot_tn(pl_low, stack(do)).astype(BF16)
    loop(pairs * (tokens // 128), attention_back)
    put_vector(2, colsum(gmix[:, 0:D]))
    put_vector(3, colsum(gmix[:, 2 * D:3 * D]))
    weight_grad(0, gmix, 3 * D, 0)

    def back_qkv(i):
        dnorm[:, at(i, BN)] = dot_nt(gmix[...], wq[at(i, BN), :])
    loop(D // BN, back_qkv)
    whole = rows_total

    def ln_one_back(i, carry):
        a, b = carry
        d, dg, ds = norm_back(x_ref[at(i, RB), :].astype(F32), gain_one, dnorm[at(i, RB), :])
        igrad_ref[at(i, RB), :] = (gout[at(i, RB), :] + d) * whole
        return a + dg, b + ds
    a, b = lax.fori_loop(0, nrb, ln_one_back, (zero, zero))
    put_vector(0, a)
    put_vector(1, b)
    sent[-2].wait()
    sent[-1].wait()
    cp = pltpu.make_async_copy(vstage, grad_hbm.at[used_rows:used_rows + vstage.shape[0], :], ssem.at[0])
    cp.start()
    cp.wait()


def compute(tokens, target, mask, vectors, count, weights, whole, total_rows):
    n = tokens.shape[0]
    vm = pl.BlockSpec(memory_space=pltpu.VMEM)
    anyspace = pl.BlockSpec(memory_space=pl.ANY)
    used_rows = (3 * D * D + D * D + 2 * D * FF) // 128
    return pl.pallas_call(
        functools.partial(compute_kernel, float(whole)),
        out_shape=[jax.ShapeDtypeStruct((n, D), BF16), jax.ShapeDtypeStruct((n, D), F32),
                   jax.ShapeDtypeStruct((8, 128), F32), jax.ShapeDtypeStruct((total_rows, 128), F32)],
        in_specs=[vm] * 5 + [anyspace] * 4,
        out_specs=[vm, vm, vm, anyspace],
        scratch_shapes=[
            pltpu.VMEM((D, 3 * D), BF16), pltpu.VMEM((D, D), BF16), pltpu.VMEM((D, FF), BF16), pltpu.VMEM((D, FF), BF16),
            pltpu.VMEM((n, 3 * D), BF16), pltpu.VMEM((HEADS // 2 * (n // 128), 128, 256), F32), pltpu.VMEM((n, D), BF16),
            pltpu.VMEM((n, D), F32), pltpu.VMEM((n, FF), F32), pltpu.VMEM((n, FF), BF16), pltpu.VMEM((4, D, n), BF16),
            pltpu.VMEM((n, D), F32), pltpu.VMEM((n, D), BF16), pltpu.VMEM((n, FF), BF16), pltpu.VMEM((n, 3 * D), BF16),
            pltpu.VMEM((2, D // 2 * FF // 128, 128), F32), pltpu.VMEM((total_rows - used_rows, 128), F32),
            pltpu.SemaphoreType.DMA((4,)), pltpu.SemaphoreType.DMA((2,))],
        compiler_params=pltpu.CompilerParams(vmem_limit_bytes=67043328),
        name="layer",
    )(tokens, target, mask, vectors, count, *weights)


MATS = ((D, 3 * D), (D, D), (D, FF), (D, FF))


def shards(custom, tokens, valid_mask, target, params, first_moment, second_moment):
    devices = lax.axis_size("dp") * lax.axis_size("fsdp")
    total_rows = params.shape[0] * devices
    used_rows = sum(h * w for h, w in MATS) // 128
    mask_values = valid_mask.astype(jnp.float32)
    count = jnp.full((8, 128), jnp.sum(mask_values))
    if custom:
        *weights, vectors, count = gather(params, count, MATS, total_rows - used_rows)
    else:
        whole = collect(params)
        weights = unpack(whole)[:4]
        vectors = whole[used_rows:].astype(jnp.float32)
        count = lax.psum(count, ("dp", "fsdp"))
    activations, input_grad, squares, grad = compute(
        tokens, target, mask_values.reshape(-1, 1), vectors, count, weights, tokens.shape[0] * devices * D, total_rows
    )
    if custom:
        gradient, squares = reduce(grad, squares, params.shape[0])
        gradient = gradient[: params.shape[0]]
    else:
        gradient = reduce_rows(grad)
        squares = lax.psum(squares, ("dp", "fsdp"))
    loss = squares[0, 0] / (count[0, 0] * D)
    new_first = beta_one * first_moment + (1.0 - beta_one) * gradient
    new_second = beta_two * second_moment + (1.0 - beta_two) * gradient * gradient
    first_hat = new_first / (1.0 - beta_one**STEP)
    second_hat = new_second / (1.0 - beta_two**STEP)
    new_params = params - learn_rate * (
        first_hat / (jnp.sqrt(second_hat) + adam_epsilon) + weight_decay * params
    )
    return (activations, loss, input_grad, new_params, new_first, new_second)


def solution(mesh):
    rows = P(("dp", "fsdp"), None)
    custom = mesh.shape["dp"] == NA * NB and mesh.shape["fsdp"] == 2 * NX
    return jax.shard_map(
        functools.partial(shards, custom),
        mesh=mesh,
        in_specs=(rows, P(("dp", "fsdp")), rows, rows, rows, rows),
        out_specs=(rows, P(), rows, rows, rows, rows),
        check_vma=False,
    )
```

```python
import functools
import math

import jax
import jax.numpy as jnp
from jax import lax
from jax.experimental import pallas as pl
from jax.experimental.pallas import tpu as pltpu
from jax.sharding import PartitionSpec as P

D = 768
HEADS = 12
HEAD = 64
FF = 3072
FRAMES = 16
STEP = 10


norm_epsilon = 1e-06
adam_epsilon = 1e-08
beta_one = 0.9
beta_two = 0.999
learn_rate = 0.1
weight_decay = 0.05

def unpack(tiled):
    flat = tiled.reshape(-1)
    layout = [(D, 3 * D), (D, D), (D, FF), (D, FF)]
    pieces = []
    offset = 0
    for height, breadth in layout:
        pieces.append(flat[offset : offset + height * breadth].reshape(height, breadth))
        offset = offset + height * breadth
    for length in [D] * 8 + [FF]:
        pieces.append(flat[offset : offset + length].astype(jnp.float32))
        offset = offset + length
    return pieces


def collect(shard):
    lowered = shard.astype(jnp.bfloat16)
    whole = lax.all_gather(lowered, ("dp", "fsdp"), axis=0, tiled=True)
    return whole


def reduce_rows(full):
    summed = lax.psum_scatter(full, ("dp", "fsdp"), scatter_dimension=0, tiled=True)
    return summed


MESH = pl.DeviceIdType.MESH
NA, NB, NX = 4, 2, 2
ORDERS = ((0, 1, 2), (0, 2, 1), (1, 2, 0))


def coords():
    dp = lax.axis_index("dp")
    fs = lax.axis_index("fsdp")
    return (dp // NB, dp % NB, fs // 2), fs % 2


def device(pos, core):
    return (pos[0] * NB + pos[1], pos[2] * 2 + core)


def flat(pos, core):
    return ((pos[0] * NB + pos[1]) * NX + pos[2]) * 2 + core


def steps():
    out = []
    for da in range(-(NA - 1), NA):
        for db in range(2):
            for dx in range(2):
                out.append((abs(da) + db + dx, (da, db, dx)))
    out.sort(key=lambda t: t[0])
    return [r for _, r in out]


def children(rel, order, pos):
    last = -1
    for i, d in enumerate(order):
        if rel[d] != 0:
            last = i
    res = []

    def line(up):
        a = pos[0]
        if up:
            return (a + 1 < NA, (a + 1, pos[1], pos[2]), 0)
        return (a - 1 >= 0, (a - 1, pos[1], pos[2]), 1)

    def flip(d):
        p = list(pos)
        p[d] = 1 - p[d]
        return (None, tuple(p), 1 + d)

    if last >= 0 and order[last] == 0:
        res.append(line(rel[0] < 0))
    for i in range(last + 1, 3):
        d = order[i]
        if d == 0:
            res.append(line(True))
            res.append(line(False))
        else:
            res.append(flip(d))
    return res


def source_of(rel, pos):
    a = pos[0] + rel[0]
    valid = None
    if rel[0] > 0:
        valid = a < NA
    if rel[0] < 0:
        valid = a >= 0
    return valid, (a, (pos[1] + rel[1]) % 2, (pos[2] + rel[2]) % 2)


def when(cond, fn):
    if cond is None:
        fn()
    else:
        pl.when(cond)(fn)


def both(a, b):
    if a is None:
        return b
    if b is None:
        return a
    return jnp.logical_and(a, b)


def split_rows(rows, shares):
    tiles = rows // 16
    first = int(round(tiles * shares))
    return ((0, first * 16), (first * 16, first * 16), (2 * first * 16, rows - 2 * first * 16))


F32, BF16 = jnp.float32, jnp.bfloat16
SHARE = 0.389


def greet(pos, core):
    sem = pltpu.get_barrier_semaphore()
    a, b, x = pos
    fixed = [device(pos, 1 - core), device((a, 1 - b, x), core), device((a, b, 1 - x), core),
             device(((a + 2) % NA, b, x), core)]
    for d in fixed:
        pl.semaphore_signal(sem, inc=1, device_id=d, device_id_type=MESH)
    up, down = a + 1 < NA, a - 1 >= 0
    when(up, lambda: pl.semaphore_signal(sem, inc=1, device_id=device((a + 1, b, x), core), device_id_type=MESH))
    when(down, lambda: pl.semaphore_signal(sem, inc=1, device_id=device((a - 1, b, x), core), device_id_type=MESH))
    pl.semaphore_wait(sem, len(fixed) + up.astype(jnp.int32) + down.astype(jnp.int32))


class Total:
    def __init__(self, pos, core, buf, send, recv):
        a, b, x = pos
        flip = a + 1 - 2 * (a % 2)
        partners = [device(pos, 1 - core), device((a, b, 1 - x), core), device((a, 1 - b, x), core),
                    device((flip, b, x), core), device(((a + 2) % NA, b, x), core)]
        self.buf = buf
        self.copies = [pltpu.make_async_remote_copy(
            src_ref=buf.at[2 * i], dst_ref=buf.at[2 * i + 1], send_sem=send.at[i], recv_sem=recv.at[i],
            device_id=p, device_id_type=MESH) for i, p in enumerate(partners)]
        self.n = len(partners)

    def start(self, i):
        self.copies[i].start()

    def end(self, i):
        self.copies[i].wait()
        self.buf[2 * i + 2] = self.buf[2 * i] + self.buf[2 * i + 1]

    def hooks(self, first, gap):
        table = {}
        for i in range(self.n):
            table.setdefault(first + i * gap, []).append(functools.partial(self.start, i))
            table.setdefault(first + i * gap + gap - 2, []).append(functools.partial(self.end, i))
        return table


def gather_kernel(parts, rows, mats, own_ref, mask_ref, *refs):
    nm = len(mats)
    outs, vec_ref, total_ref = refs[:nm], refs[nm], refs[nm + 1]
    slots, flat_ref, send, recv, tbuf, tsend, trecv, osem = refs[nm + 2:nm + 10]
    mat_refs = refs[nm + 10:]
    pos, core = coords()
    me = flat(pos, core)
    slots[me, 0:rows, :] = own_ref[...].astype(BF16)
    if slots.shape[1] > rows:
        slots[me, rows:, :] = jnp.zeros((slots.shape[1] - rows, 128), BF16)
    tbuf[0] = jnp.full(tbuf.shape[1:], jnp.sum(mask_ref[...].astype(F32)))
    total = Total(pos, core, tbuf, tsend, trecv)
    greet(pos, core)
    hooks = total.hooks(6, 14)
    plan = steps()
    order_k = []
    for rel in plan:
        for col in range(3):
            order_k.append((rel, col))

    def chunk(idx, col):
        lo, n = parts[col]
        return slots.at[idx, pl.ds(lo, n), :]

    def copy(idx, col, k, direction, to):
        return pltpu.make_async_remote_copy(
            src_ref=chunk(idx, col), dst_ref=chunk(idx, col),
            send_sem=send.at[k, direction], recv_sem=recv.at[idx, col],
            device_id=to, device_id_type=MESH)

    def widen(idx):
        base = pl.multiple_of(idx * rows, 8)
        def body(i, _):
            r = pl.multiple_of(i * 112, 16)
            flat_ref[pl.ds(pl.multiple_of(base + r, 8), 112), :] = slots[idx, pl.ds(r, 112), :].astype(F32)
            return 0
        lax.fori_loop(0, rows // 112, body, 0)
        rest = rows % 112
        if rest:
            r = rows // 112 * 112
            flat_ref[pl.ds(pl.multiple_of(base + r, 8), rest), :] = slots[idx, r:r + rest, :].astype(F32)

    def run(k, rel, col, valid, src):
        def inner():
            idx = flat(src, core)
            if rel != (0, 0, 0):
                copy(idx, col, k, 0, device(pos, 1 - core)).wait_recv()
            for cond, child, direction in children(rel, ORDERS[col], pos):
                when(cond, lambda child=child, direction=direction: copy(idx, col, k, direction, device(child, core)).start())
            copy(idx, col, k, 4, device(pos, 1 - core)).start()
        when(valid, inner)

    def sibling(rel, k0):
        valid, src = source_of(rel, pos)
        def inner():
            other = flat(src, 1 - core)
            for col in range(3):
                copy(other, col, k0 + col, 4, device(pos, 1 - core)).wait_recv()
            widen(flat(src, core))
            widen(other)
        when(valid, inner)

    def finish(k, rel, col, valid, src):
        def inner():
            idx = flat(src, core)
            for cond, child, direction in children(rel, ORDERS[col], pos):
                when(cond, lambda child=child, direction=direction: copy(idx, col, k, direction, device(child, core)).wait_send())
            copy(idx, col, k, 4, device(pos, 1 - core)).wait_send()
        when(valid, inner)

    LAG = 2
    for i, rel in enumerate(plan):
        valid, src = source_of(rel, pos)
        for col in range(3):
            k = 3 * i + col
            run(k, rel, col, valid, src)
            for h in hooks.get(k, ()):
                h()
        if i >= LAG:
            sibling(plan[i - LAG], 3 * (i - LAG))
    for i in range(len(plan) - LAG, len(plan)):
        sibling(plan[i], 3 * i)
    total_ref[...] = tbuf[2 * total.n]
    first = 0
    copies = []
    for (height, width), mat, out, s in zip(mats, mat_refs, outs, range(nm)):
        n = width // 128
        def body(i, _, mat=mat, n=n, first=first):
            r = pl.multiple_of(i * 16, 16)
            for j in range(n):
                mat[pl.ds(r, 16), 128 * j:128 * (j + 1)] = flat_ref[pl.ds(first + r * n + j, 16, stride=n), :].astype(BF16)
            return 0
        lax.fori_loop(0, height // 16, body, 0)
        cp = pltpu.make_async_copy(mat, out, osem.at[s])
        cp.start()
        copies.append(cp)
        first += height * n
    vec_ref[...] = flat_ref[first:first + vec_ref.shape[0], :]
    for i, rel in enumerate(plan):
        valid, src = source_of(rel, pos)
        for col in range(3):
            finish(3 * i + col, rel, col, valid, src)
    for cp in copies:
        cp.wait()


def gather(own, mask, mats, vec_rows):
    rows = own.shape[0]
    devices = 2 * NA * NB * NX
    slot = (rows + 15) // 16 * 16
    parts = split_rows(slot, SHARE)
    vm = pl.BlockSpec(memory_space=pltpu.VMEM)
    outs = [jax.ShapeDtypeStruct(m, BF16) for m in mats] + [
        jax.ShapeDtypeStruct((vec_rows, 128), F32), jax.ShapeDtypeStruct((8, 128), F32)]
    return pl.pallas_call(
        functools.partial(gather_kernel, parts, rows, mats),
        out_shape=outs,
        in_specs=[vm, vm],
        out_specs=[pl.BlockSpec(memory_space=pl.ANY)] * len(mats) + [vm, vm],
        scratch_shapes=[
            pltpu.VMEM((devices, slot, 128), BF16), pltpu.VMEM((devices * rows, 128), F32),
            pltpu.SemaphoreType.DMA((84, 5)), pltpu.SemaphoreType.DMA((devices, 3)),
            pltpu.VMEM((11, 8, 128), F32), pltpu.SemaphoreType.DMA((5,)), pltpu.SemaphoreType.DMA((5,)),
            pltpu.SemaphoreType.DMA((len(mats),))] + [pltpu.VMEM(m, BF16) for m in mats],
        compiler_params=pltpu.CompilerParams(collective_id=0, has_side_effects=True, vmem_limit_bytes=67043328),
        name="gather_params",
    )(own, mask)


def sweep(n, body, block=112):
    if n // block:
        def step(i, carry):
            body(pl.multiple_of(i * block, 16), block)
            return carry
        lax.fori_loop(0, n // block, step, 0)
    if n % block:
        body(n // block * block, n % block)


def reduce_kernel(parts, rows, grad_ref, part_ref, count_ref, out_ref, loss_ref, part, rb_core, rb_x, rb_b, rb_a01, rb_a2, stage, acc,
                  ssem, send_c, recv_c, send_p, recv_x, recv_b, recv_a, tbuf, tsend, trecv):
    pos, core = coords()
    plan = list(reversed(steps()))
    depth = stage.shape[0]
    loads = []
    for rel in plan:
        loads.append((rel, 1))
        loads.append((rel, 0))

    def load(i):
        rel, other = loads[i]
        valid, src = source_of(rel, pos)
        o = flat(src, 1 - core if other else core)
        return valid, o, pltpu.make_async_copy(grad_ref.at[pl.ds(pl.multiple_of(o * rows, 8), rows), :], stage.at[i % depth, 0:rows, :], ssem.at[i % depth])

    def start_load(i):
        valid, o, cp = load(i)
        when(valid, cp.start)

    tbuf[0] = part_ref[...]
    for i in range(depth):
        start_load(i)
    if stage.shape[1] > rows:
        for i in range(depth):
            stage[i, rows:, :] = jnp.zeros((stage.shape[1] - rows, 128), F32)
    total = Total(pos, core, tbuf, tsend, trecv)
    greet(pos, core)
    hooks = total.hooks(6, 14)

    def core_copy(rel):
        valid, src = source_of(rel, pos)
        chip = flat(src, 0) // 2
        return valid, src, pltpu.make_async_remote_copy(
            src_ref=part.at[flat(src, 1 - core)], dst_ref=rb_core.at[chip], send_sem=send_c.at[chip], recv_sem=recv_c.at[chip],
            device_id=device(pos, 1 - core), device_id_type=MESH)

    def convert(i):
        rel, other = loads[i]
        valid, o, cp = load(i)

        def inner():
            cp.wait()
            def body(r, m):
                part[o, pl.ds(r, m), :] = stage[i % depth, pl.ds(r, m), :].astype(BF16)
            sweep(part.shape[1], body)
        when(valid, inner)

    def buffer(direction, src, col):
        lo, n = parts[col]
        if direction == 3:
            return rb_x.at[src[0] * NB + src[1], pl.ds(lo, n), :], recv_x.at[src[0] * NB + src[1], col]
        if direction == 2:
            return rb_b.at[src[0] * NX + src[2], pl.ds(lo, n), :], recv_b.at[src[0] * NX + src[2], col]
        chip = (src[0] * NB + src[1]) * NX + src[2]
        if col == 2:
            return rb_a2.at[direction, chip], recv_a.at[direction, chip, col]
        return rb_a01.at[direction, src[0], pl.ds(lo, n), :], recv_a.at[direction, chip, col]

    def parent_copy(rel, col, k, src):
        order = ORDERS[col]
        d = [d for d in order if rel[d] != 0][-1]
        to = list(pos)
        if d == 0:
            direction = 0 if rel[0] < 0 else 1
            to[0] = pos[0] - 1 if rel[0] < 0 else pos[0] + 1
        else:
            direction = 1 + d
            to[d] = 1 - pos[d]
        lo, n = parts[col]
        dst, sem = buffer(direction, src, col)
        return pltpu.make_async_remote_copy(
            src_ref=part.at[flat(src, core), pl.ds(lo, n), :], dst_ref=dst, send_sem=send_p.at[k], recv_sem=sem,
            device_id=device(to, core), device_id_type=MESH)

    def arrived(direction, src, col):
        dst, sem = buffer(direction, src, col)
        return pltpu.make_async_remote_copy(src_ref=dst, dst_ref=dst, send_sem=send_p.at[0], recv_sem=sem,
                                            device_id=device(pos, 1 - core), device_id_type=MESH)

    def combine(k, rel, col):
        valid, src = source_of(rel, pos)
        lo, n = parts[col]

        def inner():
            o = flat(src, core)
            chip = flat(src, 0) // 2
            if col == 0:
                core_copy(rel)[2].wait_recv()
            kids = children(rel, ORDERS[col], pos)
            sure = [d for c, _, d in kids if c is None]
            maybe = [(c, d) for c, _, d in kids if c is not None]
            for d in sure:
                arrived(d, src, col).wait_recv()
            refs = [buffer(d, src, col)[0] for d in sure]

            def fold(write):
                def body(r, m):
                    v = part[o, pl.ds(lo + r, m), :].astype(F32) + rb_core[chip, pl.ds(lo + r, m), :].astype(F32)
                    for ref in refs:
                        v = v + ref[pl.ds(r, m), :].astype(F32)
                    write(r, m, v)
                sweep(n, body)

            root = rel == (0, 0, 0)

            def emit(r, m, v):
                if root:
                    out_ref[pl.ds(lo + r, m), :] = v
                else:
                    part[o, pl.ds(lo + r, m), :] = v.astype(BF16)

            def to_acc(r, m, v):
                acc[pl.ds(r, m), :] = v

            if not maybe:
                fold(emit)
            else:
                fold(to_acc)
                for c, d in maybe:
                    def add(d=d):
                        arrived(d, src, col).wait_recv()
                        ref = buffer(d, src, col)[0]
                        def body(r, m):
                            acc[pl.ds(r, m), :] = acc[pl.ds(r, m), :] + ref[pl.ds(r, m), :].astype(F32)
                        sweep(n, body)
                    when(c, add)
                def last(r, m):
                    emit(r, m, acc[pl.ds(r, m), :])
                sweep(n, last)
            if not root:
                parent_copy(rel, col, k, src).start()
        when(valid, inner)

    AHEAD = 4
    def prepare(j):
        for i in (2 * j, 2 * j + 1):
            convert(i)
            if i + depth < len(loads):
                start_load(i + depth)
            if i % 2 == 0:
                valid, src, cp = core_copy(plan[j])
                when(valid, cp.start)
    for j in range(AHEAD):
        prepare(j)
    for j in range(len(plan)):
        if j + AHEAD < len(plan):
            prepare(j + AHEAD)
        for col in range(3):
            combine(3 * j + col, plan[j], col)
            for h in hooks.get(3 * j + col, ()):
                h()
    quotient = tbuf[2 * total.n] / (count_ref[...] * D)
    loss_ref[0, 0] = quotient[0, 0]
    for j, rel in enumerate(plan):
        valid, src, cp = core_copy(rel)
        when(valid, cp.wait_send)
        if rel != (0, 0, 0):
            for col in range(3):
                when(valid, parent_copy(rel, col, 3 * j + col, src).wait_send)


def reduce(grad, part, count, rows):
    devices = 2 * NA * NB * NX
    slot = (rows + 15) // 16 * 16
    parts = split_rows(slot, SHARE)
    two = parts[0][1] + parts[1][1]
    vm = pl.BlockSpec(memory_space=pltpu.VMEM)
    return pl.pallas_call(
        functools.partial(reduce_kernel, parts, rows),
        out_shape=[jax.ShapeDtypeStruct((slot, 128), F32), jax.ShapeDtypeStruct((1, 1), F32)],
        in_specs=[pl.BlockSpec(memory_space=pl.ANY), vm, vm],
        out_specs=[vm, pl.BlockSpec(memory_space=pltpu.SMEM)],
        scratch_shapes=[
            pltpu.VMEM((devices, slot, 128), BF16), pltpu.VMEM((devices // 2, slot, 128), BF16),
            pltpu.VMEM((NA * NB, slot, 128), BF16), pltpu.VMEM((NA * NX, slot, 128), BF16),
            pltpu.VMEM((2, NA, two, 128), BF16), pltpu.VMEM((2, devices // 2, parts[2][1], 128), BF16),
            pltpu.VMEM((4, slot, 128), F32), pltpu.VMEM((max(p[1] for p in parts), 128), F32),
            pltpu.SemaphoreType.DMA((4,)), pltpu.SemaphoreType.DMA((devices // 2,)), pltpu.SemaphoreType.DMA((devices // 2,)),
            pltpu.SemaphoreType.DMA((84,)), pltpu.SemaphoreType.DMA((NA * NB, 3)), pltpu.SemaphoreType.DMA((NA * NX, 3)),
            pltpu.SemaphoreType.DMA((2, devices // 2, 3)),
            pltpu.VMEM((11, 8, 128), F32), pltpu.SemaphoreType.DMA((5,)), pltpu.SemaphoreType.DMA((5,))],
        compiler_params=pltpu.CompilerParams(collective_id=1, has_side_effects=True, vmem_limit_bytes=67043328),
        name="reduce_gradient",
    )(grad, part, count)


TILES = 12

def dot(a, b):
    return jnp.dot(a, b, preferred_element_type=F32)


def dot_nt(a, b):
    return lax.dot_general(a, b, (((1,), (1,)), ((), ())), preferred_element_type=F32)


def dot_tn(a, b):
    return lax.dot_general(a, b, (((0,), (0,)), ((), ())), preferred_element_type=F32)


def loop(n, body):
    def step(i, carry):
        body(i)
        return carry
    lax.fori_loop(0, n, step, 0)


def several(n, body):
    def group(i):
        for j in range(TILES):
            body(i * TILES + j)
    loop(n // TILES, group)


def at(i, size):
    return pl.ds(i * size if isinstance(i, int) else pl.multiple_of(i * size, size), size)


def compute_kernel(rows_total, x_ref, target_ref, mask_ref, vec_ref, count_ref, wq_hbm, wp_hbm, wi_hbm, wo_hbm,
                   act_ref, igrad_ref, sq_ref, grad_hbm,
                   wq, wp, wi, wo, mixed, probs, att, middle, slope, active, left, gout, glow, ghid, gmix, stage, vstage, wsem, ssem):
    tokens = x_ref.shape[0]
    scale = HEAD ** (-0.5)
    loads = [pltpu.make_async_copy(h, w, wsem.at[i]) for i, (h, w) in enumerate(
        ((wq_hbm, wq), (wp_hbm, wp), (wi_hbm, wi), (wo_hbm, wo)))]
    loads[0].start()
    used_rows = (3 * D * D + D * D + 2 * D * FF) // 128

    def vector(row, n):
        return jnp.concatenate([vec_ref[row + j:row + j + 1, :] for j in range(n)], axis=1)

    per = D // 128
    gain_one, shift_one, bias_query, bias_value, bias_proj, gain_two, shift_two, bias_out = [
        vector(per * i, per) for i in range(8)]
    bias_in_row = 8 * per
    vstage[...] = jnp.zeros_like(vstage)

    def put_vector(i, v):
        for j in range(v.shape[1] // 128):
            vstage[per * i + j:per * i + j + 1, :] = v[:, 128 * j:128 * (j + 1)]

    def stats(v):
        mean = jnp.mean(v, -1, keepdims=True)
        center = v - mean
        r = lax.rsqrt(jnp.mean(center * center, -1, keepdims=True) + norm_epsilon)
        return center * r, r

    RB = 256
    nrb = tokens // RB
    low = glow

    def flip(dst):
        def body(i):
            left[dst, at(i, 128), :] = low[:, at(i, 128)].T
        loop(D // 128, body)

    def ln_one(i):
        z, _ = stats(x_ref[at(i, RB), :].astype(F32))
        low[at(i, RB), :] = (z * gain_one + shift_one).astype(BF16)
    loop(nrb, ln_one)
    loads[0].wait()
    for c in loads[1:]:
        c.start()
    BN = 256
    WN = 768
    HN = 768
    GN = 768
    SN = 256
    QN = 768
    IN = 256

    def qkv(part, bias):
        def body(i):
            j = i + part * (D // QN)
            v = dot(low[...], wq[:, at(j, QN)])
            if bias is not None:
                v = v + vec_bias[0:1, at(i, QN)]
            mixed[:, at(j, QN)] = v.astype(BF16)
        loop(D // QN, body)
    vec_bias = middle
    middle[0:1, :] = bias_query
    qkv(0, True)
    qkv(1, None)
    middle[0:1, :] = bias_value
    qkv(2, True)
    flip(0)

    pairs = HEADS // 2
    lane = lax.broadcasted_iota(jnp.int32, (128, 128), 1)
    lower = lane < HEAD
    r256 = lax.broadcasted_iota(jnp.int32, (128, 256), 0) // FRAMES
    c256 = (lax.broadcasted_iota(jnp.int32, (128, 256), 1) % 128) // FRAMES
    same = r256 == c256

    def stack(v):
        zero = jnp.zeros_like(v)
        return jnp.concatenate([jnp.where(lower, v, zero), jnp.where(lower, zero, v)], axis=0)

    def tile(i):
        g, p = i // pairs, i % pairs
        rows = at(g, 128)
        return rows, p

    def attention(i):
        rows, p = tile(i)
        q = mixed[rows, at(p, 128)]
        k = mixed[rows, at(p + pairs, 128)]
        v = mixed[rows, at(p + 2 * pairs, 128)]
        s = dot_nt(q, stack(k)) * scale
        s = jnp.where(same, s, -1e30)
        out = []
        for h in range(2):
            sh = s[:, 128 * h:128 * (h + 1)]
            e = jnp.exp(sh - jnp.max(sh, -1, keepdims=True))
            out.append(e / jnp.sum(e, -1, keepdims=True))
        pr = jnp.concatenate(out, axis=1)
        probs[i] = pr
        att[rows, at(p, 128)] = dot(pr.astype(BF16), stack(v)).astype(BF16)
    several(pairs * (tokens // 128), attention)

    loads[1].wait()

    def project(i):
        v = dot(att[at(i, RB), :], wp[...])
        m = x_ref[at(i, RB), :].astype(F32) + (v + bias_proj)
        middle[at(i, RB), :] = m
        z, _ = stats(m)
        low[at(i, RB), :] = (z * gain_two + shift_two).astype(BF16)
    loop(nrb, project)
    loads[2].wait()

    def hidden(i):
        bias = jnp.concatenate([vec_ref[pl.ds(bias_in_row + HN // 128 * i + j, 1), :] for j in range(HN // 128)], axis=1)
        h = dot(low[...], wi[:, at(i, HN)]) + bias
        cdf = 0.5 * (1.0 + lax.erf(h * (0.5 ** 0.5)))
        pdf = jnp.exp(-0.5 * h * h) * (1.0 / math.sqrt(2.0 * math.pi))
        active[:, at(i, HN)] = (h * cdf).astype(BF16)
        slope[:, at(i, HN)] = cdf + h * pdf
    loop(FF // HN, hidden)
    flip(2)
    loads[3].wait()

    def second(i):
        gout[:, at(i, SN)] = dot_nt(active[...], wo[at(i, SN), :])
    loop(D // SN, second)
    factor = 2.0 / (count_ref[0:1, 0:1] * D)
    sq_ref[...] = jnp.zeros_like(sq_ref)

    mask_columns = mask_ref[...].astype(F32).T

    def finish(i):
        o = middle[at(i, RB), :] + (gout[at(i, RB), :] + bias_out)
        act_ref[at(i, RB), :] = o.astype(BF16)
        misfit = o - target_ref[at(i, RB), :].astype(F32)
        m = jnp.concatenate([mask_columns[:, RB // 128 * i + j:RB // 128 * i + j + 1] for j in range(RB // 128)], axis=0)
        sq_ref[...] += jnp.full(sq_ref.shape, jnp.sum(m * jnp.sum(misfit * misfit, -1, keepdims=True)))
        g = (factor * m) * misfit
        gout[at(i, RB), :] = g
        low[at(i, RB), :] = g.astype(BF16)
    for i in range(nrb):
        finish(i)
    flip(3)

    def colsum(ref):
        return jnp.sum(ref.astype(F32), 0, keepdims=True)

    put_vector(7, colsum(low[...]))

    sent = []

    def weight_grad(lhs, rhs, width, first):
        n = width // 128
        half = D // 2
        for h in range(2):
            slot = len(sent) % 2
            if len(sent) >= 2:
                sent[-2].wait()
            size = half * n

            def body(j):
                v = dot(left[lhs, h * half:(h + 1) * half, :], rhs[:, at(j, WN)])
                for t in range(WN // 128):
                    stage[slot, pl.ds(WN // 128 * j + t, half, stride=n), :] = v[:, 128 * t:128 * (t + 1)]
            loop(width // WN, body)
            cp = pltpu.make_async_copy(stage.at[slot, 0:size, :], grad_hbm.at[first + h * size:first + (h + 1) * size, :], ssem.at[slot])
            cp.start()
            sent.append(cp)

    row_proj = 3 * D * D // 128
    row_in = row_proj + D * D // 128
    row_out = row_in + D * FF // 128
    weight_grad(3, active, FF, row_out)

    def back_hidden(i):
        v = dot(low[...], wo[:, at(i, GN)]) * slope[:, at(i, GN)]
        b = v.astype(BF16)
        ghid[:, at(i, GN)] = b
        s = jnp.sum(b.astype(F32), 0, keepdims=True)
        for t in range(GN // 128):
            vstage[pl.ds(bias_in_row + GN // 128 * i + t, 1), :] = s[:, 128 * t:128 * (t + 1)]
    loop(FF // GN, back_hidden)
    weight_grad(2, ghid, FF, row_in)

    dnorm = igrad_ref

    def back_in(i):
        dnorm[:, at(i, SN)] = dot_nt(ghid[...], wi[at(i, SN), :])
    loop(D // SN, back_in)

    def norm_back(values, gain, dy):
        z, r = stats(values)
        dz = dy * gain
        m1 = jnp.mean(dz, -1, keepdims=True)
        m2 = jnp.mean(dz * z, -1, keepdims=True)
        return r * (dz - m1 - z * m2), jnp.sum(dy * z, 0, keepdims=True), jnp.sum(dy, 0, keepdims=True)

    zero = jnp.zeros((1, D), F32)

    def ln_two_back(i, carry):
        a, b, c = carry
        d, dg, ds = norm_back(middle[at(i, RB), :], gain_two, dnorm[at(i, RB), :])
        g = gout[at(i, RB), :] + d
        gout[at(i, RB), :] = g
        gl = g.astype(BF16)
        low[at(i, RB), :] = gl
        return a + dg, b + ds, c + jnp.sum(gl.astype(F32), 0, keepdims=True)
    a, b, c = lax.fori_loop(0, nrb, ln_two_back, (zero, zero, zero))
    put_vector(5, a)
    put_vector(6, b)
    put_vector(4, c)

    def flip_att(i):
        left[1, at(i, 128), :] = att[:, at(i, 128)].T
    loop(D // 128, flip_att)
    weight_grad(1, low, D, row_proj)

    def back_proj(i):
        att[:, at(i, BN)] = dot_nt(low[...], wp[at(i, BN), :]).astype(BF16)
    loop(D // BN, back_proj)

    def attention_back(i):
        rows, p = tile(i)
        q = mixed[rows, at(p, 128)]
        k = mixed[rows, at(p + pairs, 128)]
        v = mixed[rows, at(p + 2 * pairs, 128)]
        do = att[rows, at(p, 128)]
        pr = probs[i]
        dp = dot_nt(do, stack(v))
        out = []
        for h in range(2):
            ph, dh = pr[:, 128 * h:128 * (h + 1)], dp[:, 128 * h:128 * (h + 1)]
            out.append((ph * (dh - jnp.sum(ph * dh, -1, keepdims=True))).astype(BF16))
        gmix[rows, at(p, 128)] = (dot(jnp.concatenate(out, axis=1), stack(k)) * scale).astype(BF16)
        gmix[rows, at(p + pairs, 128)] = (dot_tn(jnp.concatenate(out, axis=0), stack(q)) * scale).astype(BF16)
        pl_low = jnp.concatenate([pr[:, :128], pr[:, 128:]], axis=0).astype(BF16)
        gmix[rows, at(p + 2 * pairs, 128)] = dot_tn(pl_low, stack(do)).astype(BF16)
    several(pairs * (tokens // 128), attention_back)
    put_vector(2, colsum(gmix[:, 0:D]))
    put_vector(3, colsum(gmix[:, 2 * D:3 * D]))
    weight_grad(0, gmix, 3 * D, 0)

    def back_qkv(i):
        dnorm[:, at(i, SN)] = dot_nt(gmix[...], wq[at(i, SN), :])
    loop(D // SN, back_qkv)
    whole = rows_total

    def ln_one_back(i, carry):
        a, b = carry
        d, dg, ds = norm_back(x_ref[at(i, RB), :].astype(F32), gain_one, dnorm[at(i, RB), :])
        igrad_ref[at(i, RB), :] = (gout[at(i, RB), :] + d) * whole
        return a + dg, b + ds
    a, b = lax.fori_loop(0, nrb, ln_one_back, (zero, zero))
    put_vector(0, a)
    put_vector(1, b)
    sent[-2].wait()
    sent[-1].wait()
    cp = pltpu.make_async_copy(vstage, grad_hbm.at[used_rows:used_rows + vstage.shape[0], :], ssem.at[0])
    cp.start()
    cp.wait()


def compute(tokens, target, mask, vectors, count, weights, whole, total_rows):
    n = tokens.shape[0]
    vm = pl.BlockSpec(memory_space=pltpu.VMEM)
    anyspace = pl.BlockSpec(memory_space=pl.ANY)
    used_rows = (3 * D * D + D * D + 2 * D * FF) // 128
    return pl.pallas_call(
        functools.partial(compute_kernel, float(whole)),
        out_shape=[jax.ShapeDtypeStruct((n, D), BF16), jax.ShapeDtypeStruct((n, D), F32),
                   jax.ShapeDtypeStruct((8, 128), F32), jax.ShapeDtypeStruct((total_rows, 128), F32)],
        in_specs=[vm] * 5 + [anyspace] * 4,
        out_specs=[vm, vm, vm, anyspace],
        scratch_shapes=[
            pltpu.VMEM((D, 3 * D), BF16), pltpu.VMEM((D, D), BF16), pltpu.VMEM((D, FF), BF16), pltpu.VMEM((D, FF), BF16),
            pltpu.VMEM((n, 3 * D), BF16), pltpu.VMEM((HEADS // 2 * (n // 128), 128, 256), F32), pltpu.VMEM((n, D), BF16),
            pltpu.VMEM((n, D), F32), pltpu.VMEM((n, FF), F32), pltpu.VMEM((n, FF), BF16), pltpu.VMEM((4, D, n), BF16),
            pltpu.VMEM((n, D), F32), pltpu.VMEM((n, D), BF16), pltpu.VMEM((n, FF), BF16), pltpu.VMEM((n, 3 * D), BF16),
            pltpu.VMEM((2, D // 2 * FF // 128, 128), F32), pltpu.VMEM((total_rows - used_rows, 128), F32),
            pltpu.SemaphoreType.DMA((4,)), pltpu.SemaphoreType.DMA((2,))],
        compiler_params=pltpu.CompilerParams(vmem_limit_bytes=67043328),
        name="layer",
    )(tokens, target, mask, vectors, count, *weights)


MATS = ((D, 3 * D), (D, D), (D, FF), (D, FF))


def shards(custom, tokens, valid_mask, target, params, first_moment, second_moment):
    devices = lax.axis_size("dp") * lax.axis_size("fsdp")
    total_rows = params.shape[0] * devices
    used_rows = sum(h * w for h, w in MATS) // 128
    mask = valid_mask.reshape(-1, 128)
    if custom:
        *weights, vectors, count = gather(params, mask, MATS, total_rows - used_rows)
    else:
        whole = collect(params)
        weights = unpack(whole)[:4]
        vectors = whole[used_rows:].astype(jnp.float32)
        count = lax.psum(jnp.full((8, 128), jnp.sum(mask.astype(jnp.float32))), ("dp", "fsdp"))
    activations, input_grad, squares, grad = compute(
        tokens, target, mask, vectors, count, weights, tokens.shape[0] * devices * D, total_rows
    )
    if custom:
        gradient, loss = reduce(grad, squares, count, params.shape[0])
        gradient, loss = gradient[: params.shape[0]], loss.reshape(())
    else:
        gradient = reduce_rows(grad)
        loss = lax.psum(squares, ("dp", "fsdp"))[0, 0] / (count[0, 0] * D)
    new_first = beta_one * first_moment + (1.0 - beta_one) * gradient
    new_second = beta_two * second_moment + (1.0 - beta_two) * gradient * gradient
    first_hat = new_first / (1.0 - beta_one**STEP)
    second_hat = new_second / (1.0 - beta_two**STEP)
    new_params = params - learn_rate * (
        first_hat / (jnp.sqrt(second_hat) + adam_epsilon) + weight_decay * params
    )
    return (activations, loss, input_grad, new_params, new_first, new_second)


def solution(mesh):
    rows = P(("dp", "fsdp"), None)
    custom = mesh.shape["dp"] == NA * NB and mesh.shape["fsdp"] == 2 * NX
    return jax.shard_map(
        functools.partial(shards, custom),
        mesh=mesh,
        in_specs=(rows, P(("dp", "fsdp")), rows, rows, rows, rows),
        out_specs=(rows, P(), rows, rows, rows, rows),
        check_vma=False,
    )
```

```python
import functools
import math

import jax
import jax.numpy as jnp
from jax import lax
from jax.experimental import pallas as pl
from jax.experimental.pallas import tpu as pltpu
from jax.sharding import PartitionSpec as P

D = 768
HEADS = 12
HEAD = 64
FF = 3072
FRAMES = 16
STEP = 10


norm_epsilon = 1e-06
adam_epsilon = 1e-08
beta_one = 0.9
beta_two = 0.999
learn_rate = 0.1
weight_decay = 0.05

def unpack(tiled):
    flat = tiled.reshape(-1)
    layout = [(D, 3 * D), (D, D), (D, FF), (D, FF)]
    pieces = []
    offset = 0
    for height, breadth in layout:
        pieces.append(flat[offset : offset + height * breadth].reshape(height, breadth))
        offset = offset + height * breadth
    for length in [D] * 8 + [FF]:
        pieces.append(flat[offset : offset + length].astype(jnp.float32))
        offset = offset + length
    return pieces


def collect(shard):
    lowered = shard.astype(jnp.bfloat16)
    whole = lax.all_gather(lowered, ("dp", "fsdp"), axis=0, tiled=True)
    return whole


def reduce_rows(full):
    summed = lax.psum_scatter(full, ("dp", "fsdp"), scatter_dimension=0, tiled=True)
    return summed


MESH = pl.DeviceIdType.MESH
NA, NB, NX = 4, 2, 2
ORDERS = ((0, 1, 2), (0, 2, 1), (1, 2, 0))


def coords():
    dp = lax.axis_index("dp")
    fs = lax.axis_index("fsdp")
    return (dp // NB, dp % NB, fs // 2), fs % 2


def device(pos, core):
    return (pos[0] * NB + pos[1], pos[2] * 2 + core)


def flat(pos, core):
    return ((pos[0] * NB + pos[1]) * NX + pos[2]) * 2 + core


def steps(later):
    out = []
    for da in range(-(NA - 1), NA):
        for db in range(2):
            for dx in range(2):
                out.append((abs(da) * 0.8 + db + dx + later(da, db, dx) * 0.01, (da, db, dx)))
    out.sort(key=lambda t: t[0])
    return [r for _, r in out]


def children(rel, order, pos):
    last = -1
    for i, d in enumerate(order):
        if rel[d] != 0:
            last = i
    res = []

    def line(up):
        a = pos[0]
        if up:
            return (a + 1 < NA, (a + 1, pos[1], pos[2]), 0)
        return (a - 1 >= 0, (a - 1, pos[1], pos[2]), 1)

    def flip(d):
        p = list(pos)
        p[d] = 1 - p[d]
        return (None, tuple(p), 1 + d)

    if last >= 0 and order[last] == 0:
        res.append(line(rel[0] < 0))
    for i in range(last + 1, 3):
        d = order[i]
        if d == 0:
            res.append(line(True))
            res.append(line(False))
        else:
            res.append(flip(d))
    return res


def source_of(rel, pos):
    a = pos[0] + rel[0]
    valid = None
    if rel[0] > 0:
        valid = a < NA
    if rel[0] < 0:
        valid = a >= 0
    return valid, (a, (pos[1] + rel[1]) % 2, (pos[2] + rel[2]) % 2)


def when(cond, fn):
    if cond is None:
        fn()
    else:
        pl.when(cond)(fn)


def both(a, b):
    if a is None:
        return b
    if b is None:
        return a
    return jnp.logical_and(a, b)


def split_rows(rows, shares):
    tiles = rows // 16
    first = int(round(tiles * shares))
    return ((0, first * 16), (first * 16, first * 16), (2 * first * 16, rows - 2 * first * 16))


F32, BF16 = jnp.float32, jnp.bfloat16
SHARE = 0.389


def greet(pos, core):
    sem = pltpu.get_barrier_semaphore()
    a, b, x = pos
    fixed = [device(pos, 1 - core), device((a, 1 - b, x), core), device((a, b, 1 - x), core),
             device(((a + 2) % NA, b, x), core)]
    for d in fixed:
        pl.semaphore_signal(sem, inc=1, device_id=d, device_id_type=MESH)
    up, down = a + 1 < NA, a - 1 >= 0
    when(up, lambda: pl.semaphore_signal(sem, inc=1, device_id=device((a + 1, b, x), core), device_id_type=MESH))
    when(down, lambda: pl.semaphore_signal(sem, inc=1, device_id=device((a - 1, b, x), core), device_id_type=MESH))
    return lambda: pl.semaphore_wait(sem, len(fixed) + up.astype(jnp.int32) + down.astype(jnp.int32))


class Total:
    def __init__(self, pos, core, buf, send, recv):
        a, b, x = pos
        flip = a + 1 - 2 * (a % 2)
        partners = [device(pos, 1 - core), device((a, b, 1 - x), core), device((a, 1 - b, x), core),
                    device((flip, b, x), core), device(((a + 2) % NA, b, x), core)]
        self.buf = buf
        self.copies = [pltpu.make_async_remote_copy(
            src_ref=buf.at[2 * i], dst_ref=buf.at[2 * i + 1], send_sem=send.at[i], recv_sem=recv.at[i],
            device_id=p, device_id_type=MESH) for i, p in enumerate(partners)]
        self.n = len(partners)

    def start(self, i):
        self.copies[i].start()

    def end(self, i):
        self.copies[i].wait()
        self.buf[2 * i + 2] = self.buf[2 * i] + self.buf[2 * i + 1]

    def hooks(self, first, gap):
        table = {}
        for i in range(self.n):
            table.setdefault(first + i * gap, []).append(functools.partial(self.start, i))
            table.setdefault(first + i * gap + gap - 2, []).append(functools.partial(self.end, i))
        return table


def gather_kernel(parts, rows, mats, own_ref, mask_ref, *refs):
    nm = len(mats)
    outs, vec_ref, total_ref = refs[:nm], refs[nm], refs[nm + 1]
    slots, flat_ref, send, recv, tbuf, tsend, trecv, osem = refs[nm + 2:nm + 10]
    mat_refs = refs[nm + 10:]
    pos, core = coords()
    me = flat(pos, core)
    greeted = greet(pos, core)
    slots[me, 0:rows, :] = own_ref[...].astype(BF16)
    if slots.shape[1] > rows:
        slots[me, rows:, :] = jnp.zeros((slots.shape[1] - rows, 128), BF16)
    tbuf[0] = jnp.full(tbuf.shape[1:], jnp.sum(mask_ref[...].astype(F32)))
    total = Total(pos, core, tbuf, tsend, trecv)
    greeted()
    hooks = total.hooks(6, 14)
    plan = steps(lambda da, db, dx: (da < 0) == ((db + dx) % 2 == 0))
    def chunk(idx, col):
        lo, n = parts[col]
        return slots.at[idx, pl.ds(lo, n), :]

    def copy(idx, col, k, direction, to):
        return pltpu.make_async_remote_copy(
            src_ref=chunk(idx, col), dst_ref=chunk(idx, col),
            send_sem=send.at[k, direction], recv_sem=recv.at[idx, col],
            device_id=to, device_id_type=MESH)

    def whole(idx, k):
        return pltpu.make_async_remote_copy(
            src_ref=slots.at[idx], dst_ref=slots.at[idx], send_sem=send.at[k, 4], recv_sem=recv.at[idx, 0],
            device_id=device(pos, 1 - core), device_id_type=MESH)

    def widen(idx):
        base = pl.multiple_of(idx * rows, 8)
        def body(i, _):
            r = pl.multiple_of(i * 112, 16)
            flat_ref[pl.ds(pl.multiple_of(base + r, 8), 112), :] = slots[idx, pl.ds(r, 112), :].astype(F32)
            return 0
        lax.fori_loop(0, rows // 112, body, 0)
        rest = rows % 112
        if rest:
            r = rows // 112 * 112
            flat_ref[pl.ds(pl.multiple_of(base + r, 8), rest), :] = slots[idx, r:r + rest, :].astype(F32)

    def run(k, rel, col, valid, src):
        def inner():
            idx = flat(src, core)
            if rel != (0, 0, 0):
                copy(idx, col, k, 0, device(pos, 1 - core)).wait_recv()
            for cond, child, direction in children(rel, ORDERS[col], pos):
                when(cond, lambda child=child, direction=direction: copy(idx, col, k, direction, device(child, core)).start())
            if col == 2:
                whole(idx, k).start()
        when(valid, inner)

    def sibling(rel, k0):
        valid, src = source_of(rel, pos)
        def inner():
            other = flat(src, 1 - core)
            whole(other, k0 + 2).wait_recv()
            widen(flat(src, core))
            widen(other)
        when(valid, inner)

    def finish(k, rel, col, valid, src):
        def inner():
            idx = flat(src, core)
            for cond, child, direction in children(rel, ORDERS[col], pos):
                when(cond, lambda child=child, direction=direction: copy(idx, col, k, direction, device(child, core)).wait_send())
            if col == 2:
                whole(idx, k).wait_send()
        when(valid, inner)

    LAG = 2
    for i, rel in enumerate(plan):
        valid, src = source_of(rel, pos)
        for col in range(3):
            k = 3 * i + col
            run(k, rel, col, valid, src)
            for h in hooks.get(k, ()):
                h()
        if i >= LAG:
            sibling(plan[i - LAG], 3 * (i - LAG))
    for i in range(len(plan) - LAG, len(plan)):
        sibling(plan[i], 3 * i)
    total_ref[...] = tbuf[2 * total.n]
    copies = []
    starts = [sum(h * w for h, w in mats[:s]) // 128 for s in range(nm + 1)]
    for s in sorted(range(nm), key=lambda s: -mats[s][0] * mats[s][1]):
        (height, width), mat, first = mats[s], mat_refs[s], starts[s]
        n = width // 128

        def body(i, _, mat=mat, n=n, first=first):
            r = pl.multiple_of(i * 16, 16)
            for j in range(n):
                mat[pl.ds(r, 16), 128 * j:128 * (j + 1)] = flat_ref[pl.ds(first + r * n + j, 16, stride=n), :].astype(BF16)
            return 0
        lax.fori_loop(0, height // 16, body, 0)
        cp = pltpu.make_async_copy(mat, outs[s], osem.at[s])
        cp.start()
        copies.append(cp)
    first = starts[nm]
    vec_ref[...] = flat_ref[first:first + vec_ref.shape[0], :]
    for i, rel in enumerate(plan):
        valid, src = source_of(rel, pos)
        for col in range(3):
            finish(3 * i + col, rel, col, valid, src)
    for cp in copies:
        cp.wait()


def gather(own, mask, mats, vec_rows):
    rows = own.shape[0]
    devices = 2 * NA * NB * NX
    slot = (rows + 15) // 16 * 16
    parts = split_rows(slot, SHARE)
    vm = pl.BlockSpec(memory_space=pltpu.VMEM)
    outs = [jax.ShapeDtypeStruct(m, BF16) for m in mats] + [
        jax.ShapeDtypeStruct((vec_rows, 128), F32), jax.ShapeDtypeStruct((8, 128), F32)]
    return pl.pallas_call(
        functools.partial(gather_kernel, parts, rows, mats),
        out_shape=outs,
        in_specs=[vm, vm],
        out_specs=[pl.BlockSpec(memory_space=pl.ANY)] * len(mats) + [vm, vm],
        scratch_shapes=[
            pltpu.VMEM((devices, slot, 128), BF16), pltpu.VMEM((devices * rows, 128), F32),
            pltpu.SemaphoreType.DMA((84, 5)), pltpu.SemaphoreType.DMA((devices, 3)),
            pltpu.VMEM((11, 8, 128), F32), pltpu.SemaphoreType.DMA((5,)), pltpu.SemaphoreType.DMA((5,)),
            pltpu.SemaphoreType.DMA((len(mats),))] + [pltpu.VMEM(m, BF16) for m in mats],
        compiler_params=pltpu.CompilerParams(collective_id=0, has_side_effects=True, vmem_limit_bytes=67043328),
        name="gather_params",
    )(own, mask)


def sweep(n, body, block=112):
    if n // block:
        def step(i, carry):
            body(pl.multiple_of(i * block, 16), block)
            return carry
        lax.fori_loop(0, n // block, step, 0)
    if n % block:
        body(n // block * block, n % block)


def reduce_kernel(parts, rows, grad_ref, part_ref, count_ref, out_ref, loss_ref, part, rb_core, rb_x, rb_b, rb_a01, rb_a2, stage, acc,
                  ssem, send_c, recv_c, send_p, recv_x, recv_b, recv_a, tbuf, tsend, trecv):
    pos, core = coords()
    plan = list(reversed(steps(lambda da, db, dx: da < 0)))
    depth = stage.shape[0]
    loads = []
    for rel in plan:
        loads.append((rel, 1))
        loads.append((rel, 0))

    def load(i):
        rel, other = loads[i]
        valid, src = source_of(rel, pos)
        o = flat(src, 1 - core if other else core)
        return valid, o, pltpu.make_async_copy(grad_ref.at[pl.ds(pl.multiple_of(o * rows, 8), rows), :], stage.at[i % depth, 0:rows, :], ssem.at[i % depth])

    def start_load(i):
        valid, o, cp = load(i)
        when(valid, cp.start)

    greeted = greet(pos, core)
    tbuf[0] = part_ref[...]
    for i in range(depth):
        start_load(i)
    if stage.shape[1] > rows:
        for i in range(depth):
            stage[i, rows:, :] = jnp.zeros((stage.shape[1] - rows, 128), F32)
    total = Total(pos, core, tbuf, tsend, trecv)
    greeted()
    hooks = total.hooks(6, 14)

    def core_copy(rel):
        valid, src = source_of(rel, pos)
        chip = flat(src, 0) // 2
        return valid, src, pltpu.make_async_remote_copy(
            src_ref=part.at[flat(src, 1 - core)], dst_ref=rb_core.at[chip], send_sem=send_c.at[chip], recv_sem=recv_c.at[chip],
            device_id=device(pos, 1 - core), device_id_type=MESH)

    def convert(i):
        rel, other = loads[i]
        valid, o, cp = load(i)

        def inner():
            cp.wait()
            def body(r, m):
                part[o, pl.ds(r, m), :] = stage[i % depth, pl.ds(r, m), :].astype(BF16)
            sweep(part.shape[1], body)
        when(valid, inner)

    def buffer(direction, src, col):
        lo, n = parts[col]
        if direction == 3:
            return rb_x.at[src[0] * NB + src[1], pl.ds(lo, n), :], recv_x.at[src[0] * NB + src[1], col]
        if direction == 2:
            return rb_b.at[src[0] * NX + src[2], pl.ds(lo, n), :], recv_b.at[src[0] * NX + src[2], col]
        chip = (src[0] * NB + src[1]) * NX + src[2]
        if col == 2:
            return rb_a2.at[direction, chip], recv_a.at[direction, chip, col]
        return rb_a01.at[direction, src[0], pl.ds(lo, n), :], recv_a.at[direction, chip, col]

    def parent_copy(rel, col, k, src):
        order = ORDERS[col]
        d = [d for d in order if rel[d] != 0][-1]
        to = list(pos)
        if d == 0:
            direction = 0 if rel[0] < 0 else 1
            to[0] = pos[0] - 1 if rel[0] < 0 else pos[0] + 1
        else:
            direction = 1 + d
            to[d] = 1 - pos[d]
        lo, n = parts[col]
        dst, sem = buffer(direction, src, col)
        return pltpu.make_async_remote_copy(
            src_ref=part.at[flat(src, core), pl.ds(lo, n), :], dst_ref=dst, send_sem=send_p.at[k], recv_sem=sem,
            device_id=device(to, core), device_id_type=MESH)

    def arrived(direction, src, col):
        dst, sem = buffer(direction, src, col)
        return pltpu.make_async_remote_copy(src_ref=dst, dst_ref=dst, send_sem=send_p.at[0], recv_sem=sem,
                                            device_id=device(pos, 1 - core), device_id_type=MESH)

    def combine(k, rel, col):
        valid, src = source_of(rel, pos)
        lo, n = parts[col]

        def inner():
            o = flat(src, core)
            chip = flat(src, 0) // 2
            if col == 0:
                core_copy(rel)[2].wait_recv()
            kids = children(rel, ORDERS[col], pos)
            sure = [d for c, _, d in kids if c is None]
            maybe = [(c, d) for c, _, d in kids if c is not None]
            for d in sure:
                arrived(d, src, col).wait_recv()
            refs = [buffer(d, src, col)[0] for d in sure]

            def fold(write):
                def body(r, m):
                    v = part[o, pl.ds(lo + r, m), :].astype(F32) + rb_core[chip, pl.ds(lo + r, m), :].astype(F32)
                    for ref in refs:
                        v = v + ref[pl.ds(r, m), :].astype(F32)
                    write(r, m, v)
                sweep(n, body)

            root = rel == (0, 0, 0)

            def emit(r, m, v):
                if root:
                    out_ref[pl.ds(lo + r, m), :] = v
                else:
                    part[o, pl.ds(lo + r, m), :] = v.astype(BF16)

            def to_acc(r, m, v):
                acc[pl.ds(r, m), :] = v

            if not maybe:
                fold(emit)
            else:
                fold(to_acc)
                for c, d in maybe:
                    def add(d=d):
                        arrived(d, src, col).wait_recv()
                        ref = buffer(d, src, col)[0]
                        def body(r, m):
                            acc[pl.ds(r, m), :] = acc[pl.ds(r, m), :] + ref[pl.ds(r, m), :].astype(F32)
                        sweep(n, body)
                    when(c, add)
                def last(r, m):
                    emit(r, m, acc[pl.ds(r, m), :])
                sweep(n, last)
            if not root:
                parent_copy(rel, col, k, src).start()
        when(valid, inner)

    AHEAD = 4
    def prepare(j):
        for i in (2 * j, 2 * j + 1):
            convert(i)
            if i + depth < len(loads):
                start_load(i + depth)
            if i % 2 == 0:
                valid, src, cp = core_copy(plan[j])
                when(valid, cp.start)
    for j in range(AHEAD):
        prepare(j)
    for j in range(len(plan)):
        if j + AHEAD < len(plan):
            prepare(j + AHEAD)
        for col in range(3):
            combine(3 * j + col, plan[j], col)
            for h in hooks.get(3 * j + col, ()):
                h()
    quotient = tbuf[2 * total.n] / (count_ref[...] * D)
    loss_ref[0, 0] = quotient[0, 0]
    for j, rel in enumerate(plan):
        valid, src, cp = core_copy(rel)
        when(valid, cp.wait_send)
        if rel != (0, 0, 0):
            for col in range(3):
                when(valid, parent_copy(rel, col, 3 * j + col, src).wait_send)


def reduce(grad, part, count, rows):
    devices = 2 * NA * NB * NX
    slot = (rows + 15) // 16 * 16
    parts = split_rows(slot, SHARE)
    two = parts[0][1] + parts[1][1]
    vm = pl.BlockSpec(memory_space=pltpu.VMEM)
    return pl.pallas_call(
        functools.partial(reduce_kernel, parts, rows),
        out_shape=[jax.ShapeDtypeStruct((slot, 128), F32), jax.ShapeDtypeStruct((1, 1), F32)],
        in_specs=[pl.BlockSpec(memory_space=pl.ANY), vm, vm],
        out_specs=[vm, pl.BlockSpec(memory_space=pltpu.SMEM)],
        scratch_shapes=[
            pltpu.VMEM((devices, slot, 128), BF16), pltpu.VMEM((devices // 2, slot, 128), BF16),
            pltpu.VMEM((NA * NB, slot, 128), BF16), pltpu.VMEM((NA * NX, slot, 128), BF16),
            pltpu.VMEM((2, NA, two, 128), BF16), pltpu.VMEM((2, devices // 2, parts[2][1], 128), BF16),
            pltpu.VMEM((4, slot, 128), F32), pltpu.VMEM((max(p[1] for p in parts), 128), F32),
            pltpu.SemaphoreType.DMA((4,)), pltpu.SemaphoreType.DMA((devices // 2,)), pltpu.SemaphoreType.DMA((devices // 2,)),
            pltpu.SemaphoreType.DMA((84,)), pltpu.SemaphoreType.DMA((NA * NB, 3)), pltpu.SemaphoreType.DMA((NA * NX, 3)),
            pltpu.SemaphoreType.DMA((2, devices // 2, 3)),
            pltpu.VMEM((11, 8, 128), F32), pltpu.SemaphoreType.DMA((5,)), pltpu.SemaphoreType.DMA((5,))],
        compiler_params=pltpu.CompilerParams(collective_id=1, has_side_effects=True, vmem_limit_bytes=67043328),
        name="reduce_gradient",
    )(grad, part, count)


TILES = 12

def dot(a, b):
    return jnp.dot(a, b, preferred_element_type=F32)


def dot_nt(a, b):
    return lax.dot_general(a, b, (((1,), (1,)), ((), ())), preferred_element_type=F32)


def dot_tn(a, b):
    return lax.dot_general(a, b, (((0,), (0,)), ((), ())), preferred_element_type=F32)


def loop(n, body):
    def step(i, carry):
        body(i)
        return carry
    lax.fori_loop(0, n, step, 0)


def several(n, body):
    def group(i):
        for j in range(TILES):
            body(i * TILES + j)
    loop(n // TILES, group)


def at(i, size):
    return pl.ds(i * size if isinstance(i, int) else pl.multiple_of(i * size, size), size)


def compute_kernel(rows_total, x_ref, target_ref, mask_ref, vec_ref, count_ref, wq_hbm, wp_hbm, wi_hbm, wo_hbm,
                   act_ref, igrad_ref, sq_ref, grad_hbm,
                   wq, wp, wi, wo, mixed, probs, att, middle, slope, active, left, gout, glow, ghid, gmix, stage, vstage, wsem, ssem):
    tokens = x_ref.shape[0]
    scale = HEAD ** (-0.5)
    loads = [pltpu.make_async_copy(h, w, wsem.at[i]) for i, (h, w) in enumerate(
        ((wq_hbm, wq), (wp_hbm, wp), (wi_hbm, wi), (wo_hbm, wo)))]
    loads[0].start()
    used_rows = (3 * D * D + D * D + 2 * D * FF) // 128

    def vector(row, n):
        return jnp.concatenate([vec_ref[row + j:row + j + 1, :] for j in range(n)], axis=1)

    per = D // 128
    gain_one, shift_one, bias_query, bias_value, bias_proj, gain_two, shift_two, bias_out = [
        vector(per * i, per) for i in range(8)]
    bias_in_row = 8 * per
    vstage[...] = jnp.zeros_like(vstage)

    def put_vector(i, v):
        for j in range(v.shape[1] // 128):
            vstage[per * i + j:per * i + j + 1, :] = v[:, 128 * j:128 * (j + 1)]

    def stats(v):
        mean = jnp.mean(v, -1, keepdims=True)
        center = v - mean
        r = lax.rsqrt(jnp.mean(center * center, -1, keepdims=True) + norm_epsilon)
        return center * r, r

    RB = 256
    nrb = tokens // RB
    low = glow

    def flip(dst):
        def body(i):
            left[dst, at(i, 128), :] = low[:, at(i, 128)].T
        loop(D // 128, body)

    def ln_one(i):
        z, _ = stats(x_ref[at(i, RB), :].astype(F32))
        low[at(i, RB), :] = (z * gain_one + shift_one).astype(BF16)
    loop(nrb, ln_one)
    loads[0].wait()
    for c in loads[1:]:
        c.start()
    BN = 256
    WN = 768
    HN = 768
    GN = 768
    SN = 256
    QN = 768
    IN = 256

    def qkv(part, bias):
        def body(i):
            j = i + part * (D // QN)
            v = dot(low[...], wq[:, at(j, QN)])
            if bias is not None:
                v = v + vec_bias[0:1, at(i, QN)]
            mixed[:, at(j, QN)] = v.astype(BF16)
        loop(D // QN, body)
    vec_bias = middle
    middle[0:1, :] = bias_query
    qkv(0, True)
    qkv(1, None)
    middle[0:1, :] = bias_value
    qkv(2, True)
    flip(0)

    pairs = HEADS // 2
    lane = lax.broadcasted_iota(jnp.int32, (128, 128), 1)
    lower = lane < HEAD
    r256 = lax.broadcasted_iota(jnp.int32, (128, 256), 0) // FRAMES
    c256 = (lax.broadcasted_iota(jnp.int32, (128, 256), 1) % 128) // FRAMES
    same = r256 == c256

    def stack(v):
        zero = jnp.zeros_like(v)
        return jnp.concatenate([jnp.where(lower, v, zero), jnp.where(lower, zero, v)], axis=0)

    def tile(i):
        g, p = i // pairs, i % pairs
        rows = at(g, 128)
        return rows, p

    def attention(i):
        rows, p = tile(i)
        q = mixed[rows, at(p, 128)]
        k = mixed[rows, at(p + pairs, 128)]
        v = mixed[rows, at(p + 2 * pairs, 128)]
        s = dot_nt(q, stack(k)) * scale
        s = jnp.where(same, s, -1e30)
        out = []
        for h in range(2):
            sh = s[:, 128 * h:128 * (h + 1)]
            e = jnp.exp(sh - jnp.max(sh, -1, keepdims=True))
            out.append(e / jnp.sum(e, -1, keepdims=True))
        pr = jnp.concatenate(out, axis=1)
        probs[i] = pr
        att[rows, at(p, 128)] = dot(pr.astype(BF16), stack(v)).astype(BF16)
    several(pairs * (tokens // 128), attention)

    loads[1].wait()

    def project(i):
        v = dot(att[at(i, RB), :], wp[...])
        m = x_ref[at(i, RB), :].astype(F32) + (v + bias_proj)
        middle[at(i, RB), :] = m
        z, _ = stats(m)
        low[at(i, RB), :] = (z * gain_two + shift_two).astype(BF16)
    loop(nrb, project)
    loads[2].wait()

    def hidden(i):
        bias = jnp.concatenate([vec_ref[pl.ds(bias_in_row + HN // 128 * i + j, 1), :] for j in range(HN // 128)], axis=1)
        h = dot(low[...], wi[:, at(i, HN)]) + bias
        cdf = 0.5 * (1.0 + lax.erf(h * (0.5 ** 0.5)))
        pdf = jnp.exp(-0.5 * h * h) * (1.0 / math.sqrt(2.0 * math.pi))
        active[:, at(i, HN)] = (h * cdf).astype(BF16)
        slope[:, at(i, HN)] = cdf + h * pdf
    loop(FF // HN, hidden)
    flip(2)
    loads[3].wait()

    def second(i):
        gout[:, at(i, SN)] = dot_nt(active[...], wo[at(i, SN), :])
    loop(D // SN, second)
    factor = 2.0 / (count_ref[0:1, 0:1] * D)
    sq_ref[...] = jnp.zeros_like(sq_ref)

    mask_columns = mask_ref[...].astype(F32).T

    def finish(i):
        o = middle[at(i, RB), :] + (gout[at(i, RB), :] + bias_out)
        act_ref[at(i, RB), :] = o.astype(BF16)
        misfit = o - target_ref[at(i, RB), :].astype(F32)
        m = jnp.concatenate([mask_columns[:, RB // 128 * i + j:RB // 128 * i + j + 1] for j in range(RB // 128)], axis=0)
        sq_ref[...] += jnp.full(sq_ref.shape, jnp.sum(m * jnp.sum(misfit * misfit, -1, keepdims=True)))
        g = (factor * m) * misfit
        gout[at(i, RB), :] = g
        low[at(i, RB), :] = g.astype(BF16)
    for i in range(nrb):
        finish(i)
    flip(3)

    def colsum(ref):
        return jnp.sum(ref.astype(F32), 0, keepdims=True)

    put_vector(7, colsum(low[...]))

    sent = []

    def weight_grad(lhs, rhs, width, first):
        n = width // 128
        half = D // 2
        for h in range(2):
            slot = len(sent) % 2
            if len(sent) >= 2:
                sent[-2].wait()
            size = half * n

            def body(j):
                v = dot(left[lhs, h * half:(h + 1) * half, :], rhs[:, at(j, WN)])
                for t in range(WN // 128):
                    stage[slot, pl.ds(WN // 128 * j + t, half, stride=n), :] = v[:, 128 * t:128 * (t + 1)]
            loop(width // WN, body)
            cp = pltpu.make_async_copy(stage.at[slot, 0:size, :], grad_hbm.at[first + h * size:first + (h + 1) * size, :], ssem.at[slot])
            cp.start()
            sent.append(cp)

    row_proj = 3 * D * D // 128
    row_in = row_proj + D * D // 128
    row_out = row_in + D * FF // 128
    weight_grad(3, active, FF, row_out)

    def back_hidden(i):
        v = dot(low[...], wo[:, at(i, GN)]) * slope[:, at(i, GN)]
        b = v.astype(BF16)
        ghid[:, at(i, GN)] = b
        s = jnp.sum(b.astype(F32), 0, keepdims=True)
        for t in range(GN // 128):
            vstage[pl.ds(bias_in_row + GN // 128 * i + t, 1), :] = s[:, 128 * t:128 * (t + 1)]
    loop(FF // GN, back_hidden)
    weight_grad(2, ghid, FF, row_in)

    dnorm = igrad_ref

    def back_in(i):
        dnorm[:, at(i, SN)] = dot_nt(ghid[...], wi[at(i, SN), :])
    loop(D // SN, back_in)

    def norm_back(values, gain, dy):
        z, r = stats(values)
        dz = dy * gain
        m1 = jnp.mean(dz, -1, keepdims=True)
        m2 = jnp.mean(dz * z, -1, keepdims=True)
        return r * (dz - m1 - z * m2), jnp.sum(dy * z, 0, keepdims=True), jnp.sum(dy, 0, keepdims=True)

    zero = jnp.zeros((1, D), F32)

    def ln_two_back(i, carry):
        a, b, c = carry
        d, dg, ds = norm_back(middle[at(i, RB), :], gain_two, dnorm[at(i, RB), :])
        g = gout[at(i, RB), :] + d
        gout[at(i, RB), :] = g
        gl = g.astype(BF16)
        low[at(i, RB), :] = gl
        return a + dg, b + ds, c + jnp.sum(gl.astype(F32), 0, keepdims=True)
    a, b, c = lax.fori_loop(0, nrb, ln_two_back, (zero, zero, zero))
    put_vector(5, a)
    put_vector(6, b)
    put_vector(4, c)

    def flip_att(i):
        left[1, at(i, 128), :] = att[:, at(i, 128)].T
    loop(D // 128, flip_att)
    weight_grad(1, low, D, row_proj)

    def back_proj(i):
        att[:, at(i, BN)] = dot_nt(low[...], wp[at(i, BN), :]).astype(BF16)
    loop(D // BN, back_proj)

    def attention_back(i):
        rows, p = tile(i)
        q = mixed[rows, at(p, 128)]
        k = mixed[rows, at(p + pairs, 128)]
        v = mixed[rows, at(p + 2 * pairs, 128)]
        do = att[rows, at(p, 128)]
        pr = probs[i]
        dp = dot_nt(do, stack(v))
        out = []
        for h in range(2):
            ph, dh = pr[:, 128 * h:128 * (h + 1)], dp[:, 128 * h:128 * (h + 1)]
            out.append((ph * (dh - jnp.sum(ph * dh, -1, keepdims=True))).astype(BF16))
        gmix[rows, at(p, 128)] = (dot(jnp.concatenate(out, axis=1), stack(k)) * scale).astype(BF16)
        gmix[rows, at(p + pairs, 128)] = (dot_tn(jnp.concatenate(out, axis=0), stack(q)) * scale).astype(BF16)
        pl_low = jnp.concatenate([pr[:, :128], pr[:, 128:]], axis=0).astype(BF16)
        gmix[rows, at(p + 2 * pairs, 128)] = dot_tn(pl_low, stack(do)).astype(BF16)
    several(pairs * (tokens // 128), attention_back)
    put_vector(2, colsum(gmix[:, 0:D]))
    put_vector(3, colsum(gmix[:, 2 * D:3 * D]))
    weight_grad(0, gmix, 3 * D, 0)

    def back_qkv(i):
        dnorm[:, at(i, SN)] = dot_nt(gmix[...], wq[at(i, SN), :])
    loop(D // SN, back_qkv)
    whole = rows_total

    def ln_one_back(i, carry):
        a, b = carry
        d, dg, ds = norm_back(x_ref[at(i, RB), :].astype(F32), gain_one, dnorm[at(i, RB), :])
        igrad_ref[at(i, RB), :] = (gout[at(i, RB), :] + d) * whole
        return a + dg, b + ds
    a, b = lax.fori_loop(0, nrb, ln_one_back, (zero, zero))
    put_vector(0, a)
    put_vector(1, b)
    sent[-2].wait()
    sent[-1].wait()
    cp = pltpu.make_async_copy(vstage, grad_hbm.at[used_rows:used_rows + vstage.shape[0], :], ssem.at[0])
    cp.start()
    cp.wait()


def compute(tokens, target, mask, vectors, count, weights, whole, total_rows):
    n = tokens.shape[0]
    vm = pl.BlockSpec(memory_space=pltpu.VMEM)
    anyspace = pl.BlockSpec(memory_space=pl.ANY)
    used_rows = (3 * D * D + D * D + 2 * D * FF) // 128
    return pl.pallas_call(
        functools.partial(compute_kernel, float(whole)),
        out_shape=[jax.ShapeDtypeStruct((n, D), BF16), jax.ShapeDtypeStruct((n, D), F32),
                   jax.ShapeDtypeStruct((8, 128), F32), jax.ShapeDtypeStruct((total_rows, 128), F32)],
        in_specs=[vm] * 5 + [anyspace] * 4,
        out_specs=[vm, vm, vm, anyspace],
        scratch_shapes=[
            pltpu.VMEM((D, 3 * D), BF16), pltpu.VMEM((D, D), BF16), pltpu.VMEM((D, FF), BF16), pltpu.VMEM((D, FF), BF16),
            pltpu.VMEM((n, 3 * D), BF16), pltpu.VMEM((HEADS // 2 * (n // 128), 128, 256), F32), pltpu.VMEM((n, D), BF16),
            pltpu.VMEM((n, D), F32), pltpu.VMEM((n, FF), F32), pltpu.VMEM((n, FF), BF16), pltpu.VMEM((4, D, n), BF16),
            pltpu.VMEM((n, D), F32), pltpu.VMEM((n, D), BF16), pltpu.VMEM((n, FF), BF16), pltpu.VMEM((n, 3 * D), BF16),
            pltpu.VMEM((2, D // 2 * FF // 128, 128), F32), pltpu.VMEM((total_rows - used_rows, 128), F32),
            pltpu.SemaphoreType.DMA((4,)), pltpu.SemaphoreType.DMA((2,))],
        compiler_params=pltpu.CompilerParams(vmem_limit_bytes=67043328),
        name="layer",
    )(tokens, target, mask, vectors, count, *weights)


MATS = ((D, 3 * D), (D, D), (D, FF), (D, FF))


def shards(custom, tokens, valid_mask, target, params, first_moment, second_moment):
    devices = lax.axis_size("dp") * lax.axis_size("fsdp")
    total_rows = params.shape[0] * devices
    used_rows = sum(h * w for h, w in MATS) // 128
    mask = valid_mask.reshape(-1, 128)
    if custom:
        *weights, vectors, count = gather(params, mask, MATS, total_rows - used_rows)
    else:
        whole = collect(params)
        weights = unpack(whole)[:4]
        vectors = whole[used_rows:].astype(jnp.float32)
        count = lax.psum(jnp.full((8, 128), jnp.sum(mask.astype(jnp.float32))), ("dp", "fsdp"))
    activations, input_grad, squares, grad = compute(
        tokens, target, mask, vectors, count, weights, tokens.shape[0] * devices * D, total_rows
    )
    if custom:
        gradient, loss = reduce(grad, squares, count, params.shape[0])
        gradient, loss = gradient[: params.shape[0]], loss.reshape(())
    else:
        gradient = reduce_rows(grad)
        loss = lax.psum(squares, ("dp", "fsdp"))[0, 0] / (count[0, 0] * D)
    new_first = beta_one * first_moment + (1.0 - beta_one) * gradient
    new_second = beta_two * second_moment + (1.0 - beta_two) * gradient * gradient
    first_hat = new_first / (1.0 - beta_one**STEP)
    second_hat = new_second / (1.0 - beta_two**STEP)
    new_params = params - learn_rate * (
        first_hat / (jnp.sqrt(second_hat) + adam_epsilon) + weight_decay * params
    )
    return (activations, loss, input_grad, new_params, new_first, new_second)


def solution(mesh):
    rows = P(("dp", "fsdp"), None)
    custom = mesh.shape["dp"] == NA * NB and mesh.shape["fsdp"] == 2 * NX
    return jax.shard_map(
        functools.partial(shards, custom),
        mesh=mesh,
        in_specs=(rows, P(("dp", "fsdp")), rows, rows, rows, rows),
        out_specs=(rows, P(), rows, rows, rows, rows),
        check_vma=False,
    )
```

```python
import functools
import math

import jax
import jax.numpy as jnp
from jax import lax
from jax.experimental import pallas as pl
from jax.experimental.pallas import tpu as pltpu
from jax.sharding import PartitionSpec as P

D = 768
HEADS = 12
HEAD = 64
FF = 3072
FRAMES = 16
STEP = 10


norm_epsilon = 1e-06
adam_epsilon = 1e-08
beta_one = 0.9
beta_two = 0.999
learn_rate = 0.1
weight_decay = 0.05

def unpack(tiled):
    flat = tiled.reshape(-1)
    layout = [(D, 3 * D), (D, D), (D, FF), (D, FF)]
    pieces = []
    offset = 0
    for height, breadth in layout:
        pieces.append(flat[offset : offset + height * breadth].reshape(height, breadth))
        offset = offset + height * breadth
    for length in [D] * 8 + [FF]:
        pieces.append(flat[offset : offset + length].astype(jnp.float32))
        offset = offset + length
    return pieces


def collect(shard):
    lowered = shard.astype(jnp.bfloat16)
    whole = lax.all_gather(lowered, ("dp", "fsdp"), axis=0, tiled=True)
    return whole


def reduce_rows(full):
    summed = lax.psum_scatter(full, ("dp", "fsdp"), scatter_dimension=0, tiled=True)
    return summed


MESH = pl.DeviceIdType.MESH
NA, NB, NX = 4, 2, 2
ORDERS = ((0, 1, 2), (0, 2, 1), (1, 2, 0))


def coords():
    dp = lax.axis_index("dp")
    fs = lax.axis_index("fsdp")
    return (dp // NB, dp % NB, fs // 2), fs % 2


def device(pos, core):
    return (pos[0] * NB + pos[1], pos[2] * 2 + core)


def flat(pos, core):
    return ((pos[0] * NB + pos[1]) * NX + pos[2]) * 2 + core


def steps(later):
    out = []
    for da in range(-(NA - 1), NA):
        for db in range(2):
            for dx in range(2):
                out.append((abs(da) * 0.8 + db + dx + later(da, db, dx) * 0.01, (da, db, dx)))
    out.sort(key=lambda t: t[0])
    return [r for _, r in out]


def children(rel, order, pos):
    last = -1
    for i, d in enumerate(order):
        if rel[d] != 0:
            last = i
    res = []

    def line(up):
        a = pos[0]
        if up:
            return (a + 1 < NA, (a + 1, pos[1], pos[2]), 0)
        return (a - 1 >= 0, (a - 1, pos[1], pos[2]), 1)

    def flip(d):
        p = list(pos)
        p[d] = 1 - p[d]
        return (None, tuple(p), 1 + d)

    if last >= 0 and order[last] == 0:
        res.append(line(rel[0] < 0))
    for i in range(last + 1, 3):
        d = order[i]
        if d == 0:
            res.append(line(True))
            res.append(line(False))
        else:
            res.append(flip(d))
    return res


def source_of(rel, pos):
    a = pos[0] + rel[0]
    valid = None
    if rel[0] > 0:
        valid = a < NA
    if rel[0] < 0:
        valid = a >= 0
    return valid, (a, (pos[1] + rel[1]) % 2, (pos[2] + rel[2]) % 2)


def when(cond, fn):
    if cond is None:
        fn()
    else:
        pl.when(cond)(fn)


def both(a, b):
    if a is None:
        return b
    if b is None:
        return a
    return jnp.logical_and(a, b)


def split_rows(rows, shares):
    tiles = rows // 16
    first = int(round(tiles * shares))
    return ((0, first * 16), (first * 16, first * 16), (2 * first * 16, rows - 2 * first * 16))


F32, BF16 = jnp.float32, jnp.bfloat16
SHARE = 0.389


def greet(pos, core):
    sem = pltpu.get_barrier_semaphore()
    a, b, x = pos
    fixed = [device(pos, 1 - core), device((a, 1 - b, x), core), device((a, b, 1 - x), core),
             device(((a + 2) % NA, b, x), core)]
    for d in fixed:
        pl.semaphore_signal(sem, inc=1, device_id=d, device_id_type=MESH)
    up, down = a + 1 < NA, a - 1 >= 0
    when(up, lambda: pl.semaphore_signal(sem, inc=1, device_id=device((a + 1, b, x), core), device_id_type=MESH))
    when(down, lambda: pl.semaphore_signal(sem, inc=1, device_id=device((a - 1, b, x), core), device_id_type=MESH))
    return lambda: pl.semaphore_wait(sem, len(fixed) + up.astype(jnp.int32) + down.astype(jnp.int32))


class Total:
    def __init__(self, pos, core, buf, send, recv):
        a, b, x = pos
        flip = a + 1 - 2 * (a % 2)
        partners = [device(pos, 1 - core), device((a, b, 1 - x), core), device((a, 1 - b, x), core),
                    device((flip, b, x), core), device(((a + 2) % NA, b, x), core)]
        self.buf = buf
        self.copies = [pltpu.make_async_remote_copy(
            src_ref=buf.at[2 * i], dst_ref=buf.at[2 * i + 1], send_sem=send.at[i], recv_sem=recv.at[i],
            device_id=p, device_id_type=MESH) for i, p in enumerate(partners)]
        self.n = len(partners)

    def start(self, i):
        self.copies[i].start()

    def end(self, i):
        self.copies[i].wait()
        self.buf[2 * i + 2] = self.buf[2 * i] + self.buf[2 * i + 1]

    def hooks(self, first, gap):
        table = {}
        for i in range(self.n):
            table.setdefault(first + i * gap, []).append(functools.partial(self.start, i))
            table.setdefault(first + i * gap + gap - 2, []).append(functools.partial(self.end, i))
        return table


def gather_kernel(parts, rows, mats, own_ref, mask_ref, *refs):
    nm = len(mats)
    outs, vec_ref, total_ref = refs[:nm], refs[nm], refs[nm + 1]
    slots, flat_ref, send, recv, tbuf, tsend, trecv, osem = refs[nm + 2:nm + 10]
    mat_refs = refs[nm + 10:]
    pos, core = coords()
    me = flat(pos, core)
    greeted = greet(pos, core)
    slots[me, 0:rows, :] = own_ref[...].astype(BF16)
    if slots.shape[1] > rows:
        slots[me, rows:, :] = jnp.zeros((slots.shape[1] - rows, 128), BF16)
    tbuf[0] = jnp.full(tbuf.shape[1:], jnp.sum(mask_ref[...].astype(F32)))
    total = Total(pos, core, tbuf, tsend, trecv)
    greeted()
    hooks = total.hooks(6, 14)
    plan = steps(lambda da, db, dx: (da < 0) == ((db + dx) % 2 == 0))
    def chunk(idx, col):
        lo, n = parts[col]
        return slots.at[idx, pl.ds(lo, n), :]

    def copy(idx, col, k, direction, to):
        return pltpu.make_async_remote_copy(
            src_ref=chunk(idx, col), dst_ref=chunk(idx, col),
            send_sem=send.at[k, direction], recv_sem=recv.at[idx, col],
            device_id=to, device_id_type=MESH)

    def whole(idx, k):
        return pltpu.make_async_remote_copy(
            src_ref=slots.at[idx], dst_ref=slots.at[idx], send_sem=send.at[k, 4], recv_sem=recv.at[idx, 0],
            device_id=device(pos, 1 - core), device_id_type=MESH)

    def widen(idx):
        base = pl.multiple_of(idx * rows, 8)
        def body(i, _):
            r = pl.multiple_of(i * 112, 16)
            flat_ref[pl.ds(pl.multiple_of(base + r, 8), 112), :] = slots[idx, pl.ds(r, 112), :].astype(F32)
            return 0
        lax.fori_loop(0, rows // 112, body, 0)
        rest = rows % 112
        if rest:
            r = rows // 112 * 112
            flat_ref[pl.ds(pl.multiple_of(base + r, 8), rest), :] = slots[idx, r:r + rest, :].astype(F32)

    def run(k, rel, col, valid, src):
        def inner():
            idx = flat(src, core)
            if rel != (0, 0, 0):
                copy(idx, col, k, 0, device(pos, 1 - core)).wait_recv()
            for cond, child, direction in children(rel, ORDERS[col], pos):
                when(cond, lambda child=child, direction=direction: copy(idx, col, k, direction, device(child, core)).start())
            if col == 2:
                whole(idx, k).start()
        when(valid, inner)

    def sibling(rel, k0):
        valid, src = source_of(rel, pos)
        def inner():
            other = flat(src, 1 - core)
            whole(other, k0 + 2).wait_recv()
            widen(flat(src, core))
            widen(other)
        when(valid, inner)

    def finish(k, rel, col, valid, src):
        def inner():
            idx = flat(src, core)
            for cond, child, direction in children(rel, ORDERS[col], pos):
                when(cond, lambda child=child, direction=direction: copy(idx, col, k, direction, device(child, core)).wait_send())
            if col == 2:
                whole(idx, k).wait_send()
        when(valid, inner)

    LAG = 2
    for i, rel in enumerate(plan):
        valid, src = source_of(rel, pos)
        for col in range(3):
            k = 3 * i + col
            run(k, rel, col, valid, src)
            for h in hooks.get(k, ()):
                h()
        if i >= LAG:
            sibling(plan[i - LAG], 3 * (i - LAG))
    for i in range(len(plan) - LAG, len(plan)):
        sibling(plan[i], 3 * i)
    total_ref[...] = tbuf[2 * total.n]
    copies = []
    starts = [sum(h * w for h, w in mats[:s]) // 128 for s in range(nm + 1)]
    for s in sorted(range(nm), key=lambda s: -mats[s][0] * mats[s][1]):
        (height, width), mat, first = mats[s], mat_refs[s], starts[s]
        n = width // 128

        def body(i, _, mat=mat, n=n, first=first):
            r = pl.multiple_of(i * 16, 16)
            for j in range(n):
                mat[pl.ds(r, 16), 128 * j:128 * (j + 1)] = flat_ref[pl.ds(first + r * n + j, 16, stride=n), :].astype(BF16)
            return 0
        lax.fori_loop(0, height // 16, body, 0)
        cp = pltpu.make_async_copy(mat, outs[s], osem.at[s])
        cp.start()
        copies.append(cp)
    first = starts[nm]
    vec_ref[...] = flat_ref[first:first + vec_ref.shape[0], :]
    for i, rel in enumerate(plan):
        valid, src = source_of(rel, pos)
        for col in range(3):
            finish(3 * i + col, rel, col, valid, src)
    for cp in copies:
        cp.wait()


def gather(own, mask, mats, vec_rows):
    rows = own.shape[0]
    devices = 2 * NA * NB * NX
    slot = (rows + 15) // 16 * 16
    parts = split_rows(slot, SHARE)
    vm = pl.BlockSpec(memory_space=pltpu.VMEM)
    outs = [jax.ShapeDtypeStruct(m, BF16) for m in mats] + [
        jax.ShapeDtypeStruct((vec_rows, 128), F32), jax.ShapeDtypeStruct((8, 128), F32)]
    return pl.pallas_call(
        functools.partial(gather_kernel, parts, rows, mats),
        out_shape=outs,
        in_specs=[vm, vm],
        out_specs=[pl.BlockSpec(memory_space=pl.ANY)] * len(mats) + [vm, vm],
        scratch_shapes=[
            pltpu.VMEM((devices, slot, 128), BF16), pltpu.VMEM((devices * rows, 128), F32),
            pltpu.SemaphoreType.DMA((84, 5)), pltpu.SemaphoreType.DMA((devices, 3)),
            pltpu.VMEM((11, 8, 128), F32), pltpu.SemaphoreType.DMA((5,)), pltpu.SemaphoreType.DMA((5,)),
            pltpu.SemaphoreType.DMA((len(mats),))] + [pltpu.VMEM(m, BF16) for m in mats],
        compiler_params=pltpu.CompilerParams(collective_id=0, has_side_effects=True, vmem_limit_bytes=67043328),
        name="gather_params",
    )(own, mask)


def sweep(n, body, block=112):
    if n // block:
        def step(i, carry):
            body(pl.multiple_of(i * block, 16), block)
            return carry
        lax.fori_loop(0, n // block, step, 0)
    if n % block:
        body(n // block * block, n % block)


def reduce_kernel(parts, rows, grad_ref, part_ref, count_ref, out_ref, loss_ref, part, rb_core, rb_x, rb_b, rb_a01, rb_a2, stage, acc,
                  ssem, send_c, recv_c, send_p, recv_x, recv_b, recv_a, tbuf, tsend, trecv):
    pos, core = coords()
    plan = list(reversed(steps(lambda da, db, dx: da < 0)))
    depth = stage.shape[0]
    loads = []
    for rel in plan:
        loads.append((rel, 1))
        loads.append((rel, 0))

    def load(i):
        rel, other = loads[i]
        valid, src = source_of(rel, pos)
        o = flat(src, 1 - core if other else core)
        return valid, o, pltpu.make_async_copy(grad_ref.at[pl.ds(pl.multiple_of(o * rows, 8), rows), :], stage.at[i % depth, 0:rows, :], ssem.at[i % depth])

    def start_load(i):
        valid, o, cp = load(i)
        when(valid, cp.start)

    greeted = greet(pos, core)
    tbuf[0] = part_ref[...]
    for i in range(depth):
        start_load(i)
    if stage.shape[1] > rows:
        for i in range(depth):
            stage[i, rows:, :] = jnp.zeros((stage.shape[1] - rows, 128), F32)
    total = Total(pos, core, tbuf, tsend, trecv)
    greeted()
    hooks = total.hooks(6, 14)

    def core_copy(rel):
        valid, src = source_of(rel, pos)
        chip = flat(src, 0) // 2
        return valid, src, pltpu.make_async_remote_copy(
            src_ref=part.at[flat(src, 1 - core)], dst_ref=rb_core.at[chip], send_sem=send_c.at[chip], recv_sem=recv_c.at[chip],
            device_id=device(pos, 1 - core), device_id_type=MESH)

    def convert(i):
        rel, other = loads[i]
        valid, o, cp = load(i)

        def inner():
            cp.wait()
            def body(r, m):
                part[o, pl.ds(r, m), :] = stage[i % depth, pl.ds(r, m), :].astype(BF16)
            sweep(part.shape[1], body)
        when(valid, inner)

    def buffer(direction, src, col):
        lo, n = parts[col]
        if direction == 3:
            return rb_x.at[src[0] * NB + src[1], pl.ds(lo, n), :], recv_x.at[src[0] * NB + src[1], col]
        if direction == 2:
            return rb_b.at[src[0] * NX + src[2], pl.ds(lo, n), :], recv_b.at[src[0] * NX + src[2], col]
        chip = (src[0] * NB + src[1]) * NX + src[2]
        if col == 2:
            return rb_a2.at[direction, chip], recv_a.at[direction, chip, col]
        return rb_a01.at[direction, src[0], pl.ds(lo, n), :], recv_a.at[direction, chip, col]

    def parent_copy(rel, col, k, src):
        order = ORDERS[col]
        d = [d for d in order if rel[d] != 0][-1]
        to = list(pos)
        if d == 0:
            direction = 0 if rel[0] < 0 else 1
            to[0] = pos[0] - 1 if rel[0] < 0 else pos[0] + 1
        else:
            direction = 1 + d
            to[d] = 1 - pos[d]
        lo, n = parts[col]
        dst, sem = buffer(direction, src, col)
        return pltpu.make_async_remote_copy(
            src_ref=part.at[flat(src, core), pl.ds(lo, n), :], dst_ref=dst, send_sem=send_p.at[k], recv_sem=sem,
            device_id=device(to, core), device_id_type=MESH)

    def arrived(direction, src, col):
        dst, sem = buffer(direction, src, col)
        return pltpu.make_async_remote_copy(src_ref=dst, dst_ref=dst, send_sem=send_p.at[0], recv_sem=sem,
                                            device_id=device(pos, 1 - core), device_id_type=MESH)

    def combine(k, rel, col):
        valid, src = source_of(rel, pos)
        lo, n = parts[col]

        def inner():
            o = flat(src, core)
            chip = flat(src, 0) // 2
            if col == 0:
                core_copy(rel)[2].wait_recv()
            kids = children(rel, ORDERS[col], pos)
            sure = [d for c, _, d in kids if c is None]
            maybe = [(c, d) for c, _, d in kids if c is not None]
            for d in sure:
                arrived(d, src, col).wait_recv()
            refs = [buffer(d, src, col)[0] for d in sure]

            def fold(write):
                def body(r, m):
                    v = part[o, pl.ds(lo + r, m), :].astype(F32) + rb_core[chip, pl.ds(lo + r, m), :].astype(F32)
                    for ref in refs:
                        v = v + ref[pl.ds(r, m), :].astype(F32)
                    write(r, m, v)
                sweep(n, body)

            root = rel == (0, 0, 0)

            def emit(r, m, v):
                if root:
                    out_ref[pl.ds(lo + r, m), :] = v
                else:
                    part[o, pl.ds(lo + r, m), :] = v.astype(BF16)

            def to_acc(r, m, v):
                acc[pl.ds(r, m), :] = v

            if not maybe:
                fold(emit)
            else:
                fold(to_acc)
                for c, d in maybe:
                    def add(d=d):
                        arrived(d, src, col).wait_recv()
                        ref = buffer(d, src, col)[0]
                        def body(r, m):
                            acc[pl.ds(r, m), :] = acc[pl.ds(r, m), :] + ref[pl.ds(r, m), :].astype(F32)
                        sweep(n, body)
                    when(c, add)
                def last(r, m):
                    emit(r, m, acc[pl.ds(r, m), :])
                sweep(n, last)
            if not root:
                parent_copy(rel, col, k, src).start()
        when(valid, inner)

    AHEAD = 4
    def prepare(j):
        for i in (2 * j, 2 * j + 1):
            convert(i)
            if i + depth < len(loads):
                start_load(i + depth)
            if i % 2 == 0:
                valid, src, cp = core_copy(plan[j])
                when(valid, cp.start)
    for j in range(AHEAD):
        prepare(j)
    for j in range(len(plan)):
        if j + AHEAD < len(plan):
            prepare(j + AHEAD)
        for col in range(3):
            combine(3 * j + col, plan[j], col)
            for h in hooks.get(3 * j + col, ()):
                h()
    quotient = tbuf[2 * total.n] / (count_ref[...] * D)
    loss_ref[0, 0] = quotient[0, 0]
    for j, rel in enumerate(plan):
        valid, src, cp = core_copy(rel)
        when(valid, cp.wait_send)
        if rel != (0, 0, 0):
            for col in range(3):
                when(valid, parent_copy(rel, col, 3 * j + col, src).wait_send)


def reduce(grad, part, count, rows):
    devices = 2 * NA * NB * NX
    slot = (rows + 15) // 16 * 16
    parts = split_rows(slot, SHARE)
    two = parts[0][1] + parts[1][1]
    vm = pl.BlockSpec(memory_space=pltpu.VMEM)
    return pl.pallas_call(
        functools.partial(reduce_kernel, parts, rows),
        out_shape=[jax.ShapeDtypeStruct((slot, 128), F32), jax.ShapeDtypeStruct((1, 1), F32)],
        in_specs=[pl.BlockSpec(memory_space=pl.ANY), vm, vm],
        out_specs=[vm, pl.BlockSpec(memory_space=pltpu.SMEM)],
        scratch_shapes=[
            pltpu.VMEM((devices, slot, 128), BF16), pltpu.VMEM((devices // 2, slot, 128), BF16),
            pltpu.VMEM((NA * NB, slot, 128), BF16), pltpu.VMEM((NA * NX, slot, 128), BF16),
            pltpu.VMEM((2, NA, two, 128), BF16), pltpu.VMEM((2, devices // 2, parts[2][1], 128), BF16),
            pltpu.VMEM((4, slot, 128), F32), pltpu.VMEM((max(p[1] for p in parts), 128), F32),
            pltpu.SemaphoreType.DMA((4,)), pltpu.SemaphoreType.DMA((devices // 2,)), pltpu.SemaphoreType.DMA((devices // 2,)),
            pltpu.SemaphoreType.DMA((84,)), pltpu.SemaphoreType.DMA((NA * NB, 3)), pltpu.SemaphoreType.DMA((NA * NX, 3)),
            pltpu.SemaphoreType.DMA((2, devices // 2, 3)),
            pltpu.VMEM((11, 8, 128), F32), pltpu.SemaphoreType.DMA((5,)), pltpu.SemaphoreType.DMA((5,))],
        compiler_params=pltpu.CompilerParams(collective_id=1, has_side_effects=True, vmem_limit_bytes=67043328),
        name="reduce_gradient",
    )(grad, part, count)


TILES = 12

def dot(a, b):
    return jnp.dot(a, b, preferred_element_type=F32)


def dot_nt(a, b):
    return lax.dot_general(a, b, (((1,), (1,)), ((), ())), preferred_element_type=F32)


def dot_tn(a, b):
    return lax.dot_general(a, b, (((0,), (0,)), ((), ())), preferred_element_type=F32)


def loop(n, body):
    def step(i, carry):
        body(i)
        return carry
    lax.fori_loop(0, n, step, 0)


def several(n, body):
    def group(i):
        for j in range(TILES):
            body(i * TILES + j)
    loop(n // TILES, group)


def at(i, size):
    return pl.ds(i * size if isinstance(i, int) else pl.multiple_of(i * size, size), size)


def compute_kernel(rows_total, x_ref, target_ref, mask_ref, vec_ref, count_ref, wq_hbm, wp_hbm, wi_hbm, wo_hbm,
                   act_ref, igrad_ref, sq_ref, grad_hbm,
                   wq, wp, wi, wo, mixed, probs, att, middle, slope, active, left, gout, glow, ghid, gmix, stage, vstage, wsem, ssem):
    tokens = x_ref.shape[0]
    scale = HEAD ** (-0.5)
    loads = [pltpu.make_async_copy(h, w, wsem.at[i]) for i, (h, w) in enumerate(
        ((wq_hbm, wq), (wp_hbm, wp), (wi_hbm, wi), (wo_hbm, wo)))]
    loads[0].start()
    used_rows = (3 * D * D + D * D + 2 * D * FF) // 128

    def vector(row, n):
        return jnp.concatenate([vec_ref[row + j:row + j + 1, :] for j in range(n)], axis=1)

    per = D // 128
    gain_one, shift_one, bias_query, bias_value, bias_proj, gain_two, shift_two, bias_out = [
        vector(per * i, per) for i in range(8)]
    bias_in_row = 8 * per
    vstage[...] = jnp.zeros_like(vstage)

    def put_vector(i, v):
        for j in range(v.shape[1] // 128):
            vstage[per * i + j:per * i + j + 1, :] = v[:, 128 * j:128 * (j + 1)]

    def stats(v):
        mean = jnp.mean(v, -1, keepdims=True)
        center = v - mean
        r = lax.rsqrt(jnp.mean(center * center, -1, keepdims=True) + norm_epsilon)
        return center * r, r

    RB = 512
    nrb = tokens // RB
    low = glow

    def flip(dst):
        def body(i):
            left[dst, at(i, 128), :] = low[:, at(i, 128)].T
        loop(D // 128, body)

    def ln_one(i):
        z, _ = stats(x_ref[at(i, RB), :].astype(F32))
        low[at(i, RB), :] = (z * gain_one + shift_one).astype(BF16)
    loop(nrb, ln_one)
    loads[0].wait()
    for c in loads[1:]:
        c.start()
    BN = 256
    WN = 768
    HN = 1536
    GN = 1536
    SN = 768
    QN = 768
    IN = 256

    def qkv(part, bias):
        def body(i):
            j = i + part * (D // QN)
            v = dot(low[...], wq[:, at(j, QN)])
            if bias is not None:
                v = v + vec_bias[0:1, at(i, QN)]
            mixed[:, at(j, QN)] = v.astype(BF16)
        loop(D // QN, body)
    vec_bias = middle
    middle[0:1, :] = bias_query
    qkv(0, True)
    qkv(1, None)
    middle[0:1, :] = bias_value
    qkv(2, True)
    flip(0)

    pairs = HEADS // 2
    lane = lax.broadcasted_iota(jnp.int32, (128, 128), 1)
    lower = lane < HEAD
    r256 = lax.broadcasted_iota(jnp.int32, (128, 256), 0) // FRAMES
    c256 = (lax.broadcasted_iota(jnp.int32, (128, 256), 1) % 128) // FRAMES
    same = r256 == c256

    def stack(v):
        zero = jnp.zeros_like(v)
        return jnp.concatenate([jnp.where(lower, v, zero), jnp.where(lower, zero, v)], axis=0)

    def tile(i):
        g, p = i // pairs, i % pairs
        rows = at(g, 128)
        return rows, p

    def attention(i):
        rows, p = tile(i)
        q = mixed[rows, at(p, 128)]
        k = mixed[rows, at(p + pairs, 128)]
        v = mixed[rows, at(p + 2 * pairs, 128)]
        s = dot_nt(q, stack(k)) * scale
        s = jnp.where(same, s, -1e30)
        out = []
        for h in range(2):
            sh = s[:, 128 * h:128 * (h + 1)]
            e = jnp.exp(sh - jnp.max(sh, -1, keepdims=True))
            out.append(e / jnp.sum(e, -1, keepdims=True))
        pr = jnp.concatenate(out, axis=1)
        probs[i] = pr
        att[rows, at(p, 128)] = dot(pr.astype(BF16), stack(v)).astype(BF16)
    several(pairs * (tokens // 128), attention)

    loads[1].wait()

    def project(i):
        v = dot(att[at(i, RB), :], wp[...])
        m = x_ref[at(i, RB), :].astype(F32) + (v + bias_proj)
        middle[at(i, RB), :] = m
        z, _ = stats(m)
        low[at(i, RB), :] = (z * gain_two + shift_two).astype(BF16)
    loop(nrb, project)
    loads[2].wait()

    def hidden(i):
        bias = jnp.concatenate([vec_ref[pl.ds(bias_in_row + HN // 128 * i + j, 1), :] for j in range(HN // 128)], axis=1)
        h = dot(low[...], wi[:, at(i, HN)]) + bias
        cdf = 0.5 * (1.0 + lax.erf(h * (0.5 ** 0.5)))
        pdf = jnp.exp(-0.5 * h * h) * (1.0 / math.sqrt(2.0 * math.pi))
        active[:, at(i, HN)] = (h * cdf).astype(BF16)
        slope[:, at(i, HN)] = cdf + h * pdf
    loop(FF // HN, hidden)
    flip(2)
    loads[3].wait()

    def second(i):
        gout[:, at(i, SN)] = dot_nt(active[...], wo[at(i, SN), :])
    loop(D // SN, second)
    factor = 2.0 / (count_ref[0:1, 0:1] * D)
    sq_ref[...] = jnp.zeros_like(sq_ref)

    mask_columns = mask_ref[...].astype(F32).T

    def finish(i):
        o = middle[at(i, RB), :] + (gout[at(i, RB), :] + bias_out)
        act_ref[at(i, RB), :] = o.astype(BF16)
        misfit = o - target_ref[at(i, RB), :].astype(F32)
        m = jnp.concatenate([mask_columns[:, RB // 128 * i + j:RB // 128 * i + j + 1] for j in range(RB // 128)], axis=0)
        sq_ref[...] += jnp.full(sq_ref.shape, jnp.sum(m * jnp.sum(misfit * misfit, -1, keepdims=True)))
        g = (factor * m) * misfit
        gout[at(i, RB), :] = g
        low[at(i, RB), :] = g.astype(BF16)
    for i in range(nrb):
        finish(i)
    flip(3)

    def colsum(ref):
        return jnp.sum(ref.astype(F32), 0, keepdims=True)

    put_vector(7, colsum(low[...]))

    sent = []

    def weight_grad(lhs, rhs, width, first):
        n = width // 128
        half = D
        for h in range(1):
            slot = 0
            if sent:
                sent[-1].wait()
            size = half * n

            def body(j):
                v = dot(left[lhs, h * half:(h + 1) * half, :], rhs[:, at(j, WN)])
                for t in range(WN // 128):
                    stage[slot, pl.ds(WN // 128 * j + t, half, stride=n), :] = v[:, 128 * t:128 * (t + 1)]
            loop(width // WN, body)
            cp = pltpu.make_async_copy(stage.at[slot, 0:size, :], grad_hbm.at[first + h * size:first + (h + 1) * size, :], ssem.at[slot])
            cp.start()
            sent.append(cp)

    row_proj = 3 * D * D // 128
    row_in = row_proj + D * D // 128
    row_out = row_in + D * FF // 128
    weight_grad(3, active, FF, row_out)

    def back_hidden(i):
        v = dot(low[...], wo[:, at(i, GN)]) * slope[:, at(i, GN)]
        b = v.astype(BF16)
        ghid[:, at(i, GN)] = b
        s = jnp.sum(b.astype(F32), 0, keepdims=True)
        for t in range(GN // 128):
            vstage[pl.ds(bias_in_row + GN // 128 * i + t, 1), :] = s[:, 128 * t:128 * (t + 1)]
    loop(FF // GN, back_hidden)
    weight_grad(2, ghid, FF, row_in)

    dnorm = igrad_ref

    def back_in(i):
        dnorm[:, at(i, SN)] = dot_nt(ghid[...], wi[at(i, SN), :])
    loop(D // SN, back_in)

    def norm_back(values, gain, dy):
        z, r = stats(values)
        dz = dy * gain
        m1 = jnp.mean(dz, -1, keepdims=True)
        m2 = jnp.mean(dz * z, -1, keepdims=True)
        return r * (dz - m1 - z * m2), jnp.sum(dy * z, 0, keepdims=True), jnp.sum(dy, 0, keepdims=True)

    zero = jnp.zeros((1, D), F32)

    def ln_two_back(i, carry):
        a, b, c = carry
        d, dg, ds = norm_back(middle[at(i, RB), :], gain_two, dnorm[at(i, RB), :])
        g = gout[at(i, RB), :] + d
        gout[at(i, RB), :] = g
        gl = g.astype(BF16)
        low[at(i, RB), :] = gl
        return a + dg, b + ds, c + jnp.sum(gl.astype(F32), 0, keepdims=True)
    a, b, c = lax.fori_loop(0, nrb, ln_two_back, (zero, zero, zero))
    put_vector(5, a)
    put_vector(6, b)
    put_vector(4, c)

    def flip_att(i):
        left[1, at(i, 128), :] = att[:, at(i, 128)].T
    loop(D // 128, flip_att)
    weight_grad(1, low, D, row_proj)

    def back_proj(i):
        att[:, at(i, BN)] = dot_nt(low[...], wp[at(i, BN), :]).astype(BF16)
    loop(D // BN, back_proj)

    def attention_back(i):
        rows, p = tile(i)
        q = mixed[rows, at(p, 128)]
        k = mixed[rows, at(p + pairs, 128)]
        v = mixed[rows, at(p + 2 * pairs, 128)]
        do = att[rows, at(p, 128)]
        pr = probs[i]
        dp = dot_nt(do, stack(v))
        out = []
        for h in range(2):
            ph, dh = pr[:, 128 * h:128 * (h + 1)], dp[:, 128 * h:128 * (h + 1)]
            out.append((ph * (dh - jnp.sum(ph * dh, -1, keepdims=True))).astype(BF16))
        gmix[rows, at(p, 128)] = (dot(jnp.concatenate(out, axis=1), stack(k)) * scale).astype(BF16)
        gmix[rows, at(p + pairs, 128)] = (dot_tn(jnp.concatenate(out, axis=0), stack(q)) * scale).astype(BF16)
        pl_low = jnp.concatenate([pr[:, :128], pr[:, 128:]], axis=0).astype(BF16)
        gmix[rows, at(p + 2 * pairs, 128)] = dot_tn(pl_low, stack(do)).astype(BF16)
    several(pairs * (tokens // 128), attention_back)
    put_vector(2, colsum(gmix[:, 0:D]))
    put_vector(3, colsum(gmix[:, 2 * D:3 * D]))
    weight_grad(0, gmix, 3 * D, 0)

    def back_qkv(i):
        dnorm[:, at(i, SN)] = dot_nt(gmix[...], wq[at(i, SN), :])
    loop(D // SN, back_qkv)
    whole = rows_total

    def ln_one_back(i, carry):
        a, b = carry
        d, dg, ds = norm_back(x_ref[at(i, RB), :].astype(F32), gain_one, dnorm[at(i, RB), :])
        igrad_ref[at(i, RB), :] = (gout[at(i, RB), :] + d) * whole
        return a + dg, b + ds
    a, b = lax.fori_loop(0, nrb, ln_one_back, (zero, zero))
    put_vector(0, a)
    put_vector(1, b)
    sent[-1].wait()
    cp = pltpu.make_async_copy(vstage, grad_hbm.at[used_rows:used_rows + vstage.shape[0], :], ssem.at[0])
    cp.start()
    cp.wait()


def compute(tokens, target, mask, vectors, count, weights, whole, total_rows):
    n = tokens.shape[0]
    vm = pl.BlockSpec(memory_space=pltpu.VMEM)
    anyspace = pl.BlockSpec(memory_space=pl.ANY)
    used_rows = (3 * D * D + D * D + 2 * D * FF) // 128
    return pl.pallas_call(
        functools.partial(compute_kernel, float(whole)),
        out_shape=[jax.ShapeDtypeStruct((n, D), BF16), jax.ShapeDtypeStruct((n, D), F32),
                   jax.ShapeDtypeStruct((8, 128), F32), jax.ShapeDtypeStruct((total_rows, 128), F32)],
        in_specs=[vm] * 5 + [anyspace] * 4,
        out_specs=[vm, vm, vm, anyspace],
        scratch_shapes=[
            pltpu.VMEM((D, 3 * D), BF16), pltpu.VMEM((D, D), BF16), pltpu.VMEM((D, FF), BF16), pltpu.VMEM((D, FF), BF16),
            pltpu.VMEM((n, 3 * D), BF16), pltpu.VMEM((HEADS // 2 * (n // 128), 128, 256), F32), pltpu.VMEM((n, D), BF16),
            pltpu.VMEM((n, D), F32), pltpu.VMEM((n, FF), F32), pltpu.VMEM((n, FF), BF16), pltpu.VMEM((4, D, n), BF16),
            pltpu.VMEM((n, D), F32), pltpu.VMEM((n, D), BF16), pltpu.VMEM((n, FF), BF16), pltpu.VMEM((n, 3 * D), BF16),
            pltpu.VMEM((1, D * FF // 128, 128), F32), pltpu.VMEM((total_rows - used_rows, 128), F32),
            pltpu.SemaphoreType.DMA((4,)), pltpu.SemaphoreType.DMA((2,))],
        compiler_params=pltpu.CompilerParams(vmem_limit_bytes=67043328),
        name="layer",
    )(tokens, target, mask, vectors, count, *weights)


MATS = ((D, 3 * D), (D, D), (D, FF), (D, FF))


def shards(custom, tokens, valid_mask, target, params, first_moment, second_moment):
    devices = lax.axis_size("dp") * lax.axis_size("fsdp")
    total_rows = params.shape[0] * devices
    used_rows = sum(h * w for h, w in MATS) // 128
    mask = valid_mask.reshape(-1, 128)
    if custom:
        *weights, vectors, count = gather(params, mask, MATS, total_rows - used_rows)
    else:
        whole = collect(params)
        weights = unpack(whole)[:4]
        vectors = whole[used_rows:].astype(jnp.float32)
        count = lax.psum(jnp.full((8, 128), jnp.sum(mask.astype(jnp.float32))), ("dp", "fsdp"))
    activations, input_grad, squares, grad = compute(
        tokens, target, mask, vectors, count, weights, tokens.shape[0] * devices * D, total_rows
    )
    if custom:
        gradient, loss = reduce(grad, squares, count, params.shape[0])
        gradient, loss = gradient[: params.shape[0]], loss.reshape(())
    else:
        gradient = reduce_rows(grad)
        loss = lax.psum(squares, ("dp", "fsdp"))[0, 0] / (count[0, 0] * D)
    new_first = beta_one * first_moment + (1.0 - beta_one) * gradient
    new_second = beta_two * second_moment + (1.0 - beta_two) * gradient * gradient
    first_hat = new_first / (1.0 - beta_one**STEP)
    second_hat = new_second / (1.0 - beta_two**STEP)
    new_params = params - learn_rate * (
        first_hat / (jnp.sqrt(second_hat) + adam_epsilon) + weight_decay * params
    )
    return (activations, loss, input_grad, new_params, new_first, new_second)


def solution(mesh):
    rows = P(("dp", "fsdp"), None)
    custom = mesh.shape["dp"] == NA * NB and mesh.shape["fsdp"] == 2 * NX
    return jax.shard_map(
        functools.partial(shards, custom),
        mesh=mesh,
        in_specs=(rows, P(("dp", "fsdp")), rows, rows, rows, rows),
        out_specs=(rows, P(), rows, rows, rows, rows),
        check_vma=False,
    )
```
